128 devices in a mesh: vocab: 32 (over z, x, y_lo), seq: 4 (over y_hi, core).
Axes of the slice: x: 4, y: 4 (y_hi: 2, y_lo: 2; y = y_hi * 2 + y_lo), z: 4, core: 2. Of those that a mesh axis runs over, the one named last changes fastest.
Arguments:
- hidden: bfloat16 [6144, 7168], P(('vocab', 'seq')), may hold values from -64 to 64
- head_matrix: bfloat16 [7168, 32768], P('seq', 'vocab'), may hold values from -4 to 4
- targets: int32 [6144], P(('vocab', 'seq')), may hold values from 0 to 32767
Outputs:
- logprob: float32 [6144], P(('vocab', 'seq'))
The draws below stay inside these ranges and needn't reach their ends.
All inputs are finite; a program needn't handle non-finite values.
Results may differ from the reference program's by a relative error of at most 0.0003.
Values may be sent and summed in bfloat16 or wider, within the bound.
No kernel may reach another device: no remote copies, remote signals or barrier semaphores. Data moves between devices by JAX's collectives and lax.ppermute only.
A program may use at most 128 MiB of HBM per device.

```python
import math
import jax
import jax.numpy as jnp
from jax import lax

D = 7168
TOK_DEV = 48
VOCAB = 32768
TOKENS = 6144
N_SEQ = 4


def head_column(key, column):
    values = jax.random.normal(jax.random.fold_in(jax.random.fold_in(key, 11), column), (D,), jnp.float32)
    values = jnp.clip(values, -4.0, 4.0)
    spread = jax.random.uniform(jax.random.fold_in(jax.random.fold_in(key, 12), column), (), jnp.float32, -0.7, 0.7)
    return values * jnp.exp(spread) * 3.0 / math.sqrt(D)


def head_columns(key, columns):

    def single(column):
        return head_column(key, column)
    return jax.vmap(single)(columns)


def draw_head_matrix(key, part):
    return head_columns(key, jnp.arange(VOCAB)).T.astype(jnp.bfloat16)


def draw_hidden(key, part):
    base_key = jax.random.fold_in(key, 21)
    return jax.random.normal(base_key, (TOKENS, D), jnp.float32).astype(jnp.bfloat16)


def with_ends(drawn, stream_key, least, high):
    spot = [jax.random.randint(jax.random.fold_in(stream_key, axis), (), 0, length) for axis, length in enumerate(drawn.shape)]
    widest = drawn.shape.index(max(drawn.shape))
    neighbour = spot[:widest] + [(spot[widest] + 1) % drawn.shape[widest]] + spot[widest + 1:]
    return drawn.at[tuple(spot)].set(least).at[tuple(neighbour)].set(high)


def setup_inputs(seed: int = 0) -> dict:
    splits = jax.random.split(jax.random.key(seed), 4)
    return {
        "hidden": draw_hidden(jax.random.fold_in(splits[3], 71), 0),
        "head_matrix": draw_head_matrix(jax.random.fold_in(splits[3], 71), 0),
        "targets": with_ends(jax.random.randint(splits[2], (TOKENS,), 0, VOCAB), jax.random.fold_in(splits[2], 1), 0, VOCAB - 1).astype(jnp.int32),
    }


def block_logprob(rows, wanted, head_matrix):
    logits = jnp.dot(rows, head_matrix, preferred_element_type=jnp.float32)
    maximum = jnp.max(logits, axis=1)
    log_total = maximum + jnp.log(jnp.sum(jnp.exp(logits - maximum[:, None]), axis=1))
    picked = jnp.take_along_axis(logits, wanted[:, None].astype(jnp.int32), axis=1)[:, 0]
    return picked - log_total


def reference(hidden, head_matrix, targets):
    block_rows = TOK_DEV * N_SEQ
    block_count = hidden.shape[0] // block_rows
    rows = hidden.reshape(block_count, block_rows, hidden.shape[1])
    wanted = targets.reshape(block_count, block_rows)

    def one_block(pieces):
        return block_logprob(pieces[0], pieces[1], head_matrix)

    results = lax.map(one_block, (rows, wanted))
    return results.reshape(-1)
```

```python
import functools

import jax
import jax.numpy as jnp
from jax import lax
from jax.experimental import pallas as pl
from jax.experimental.pallas import tpu as pltpu
from jax.sharding import Mesh
from jax.sharding import PartitionSpec as P

AXES = ("z", "x", "yl", "yh", "c")
LANES = 128
HALF = 512
MIB = 2**20


def shift(x, axis, step):
    count = lax.axis_size(axis)
    return lax.ppermute(x, axis, [(k, (k + step) % count) for k in range(count)])


def swap(x, axis):
    return lax.ppermute(x, axis, [(0, 1), (1, 0)])


def cross(x):
    return lax.ppermute(x, ("yl", "yh"), [(0, 3), (3, 0), (1, 2), (2, 1)])


def stat_kernel(rows, blocks, tile, prev_rows, unit, *refs):
    pieces = len(rows)
    scalars = refs[0]
    hidden = refs[1 : 1 + pieces]
    weights = refs[1 + pieces : 1 + pieces + 4 * blocks]
    at = 1 + pieces + 4 * blocks
    prev = None
    if prev_rows:
        prev, at = refs[at], at + 1
    out, hv, tv, wv, acc, stats, hsem, tsem, wsem = refs[at:]
    total = sum(rows)
    quarter = wv.shape[2]
    starts = [sum(rows[:k]) for k in range(pieces)]
    copies = {}
    for q in range(4):
        off = pl.multiple_of(scalars[q] * quarter, LANES)
        copies[q] = [
            pltpu.make_async_copy(weights[q], wv.at[0, q], wsem.at[q])
        ]
        for k in range(pieces):
            copies[q].append(
                pltpu.make_async_copy(
                    hidden[k].at[:, pl.ds(off, quarter)],
                    hv.at[q, pl.ds(starts[k], rows[k]), :],
                    hsem.at[q, k],
                )
            )
        for copy in copies[q]:
            copy.start()
    targets = [
        pltpu.make_async_copy(
            hidden[k].at[:, pl.ds(4 * quarter, LANES)],
            tv.at[pl.ds(starts[k], rows[k]), :],
            tsem.at[k],
        )
        for k in range(pieces)
    ]
    for copy in targets:
        copy.start()
    later = []
    for b in range(1, blocks):
        for q in range(4):
            copy = pltpu.make_async_copy(weights[4 * b + q], wv.at[b, q], wsem.at[4 * b + q])
            copy.start()
            later.append(copy)
    lane = lax.broadcasted_iota(jnp.int32, (tile, LANES), 1)
    column = lax.broadcasted_iota(jnp.int32, (tile, HALF), 1)
    if prev_rows and out.shape[0] == total:
        stats[...] = prev[...]
    for b in range(blocks):
        fresh = b == 0 and not (prev_rows and out.shape[0] == total)
        for q in range(4):
            if b == 0:
                for copy in copies[q]:
                    copy.wait()
                if q == 3:
                    for copy in targets:
                        copy.wait()
            else:
                later[4 * (b - 1) + q].wait()

            def step(r, carry, b=b, q=q, fresh=fresh):
                here = pl.ds(pl.multiple_of(r * tile, tile), tile)
                part = jnp.dot(
                    hv[q, here, :], wv[b, q], preferred_element_type=jnp.float32
                )
                if q < 3:
                    acc[here, :] = part if q == 0 else acc[here, :] + part
                    return carry
                logits = acc[here, :] + part
                ids = tv[here, :].astype(jnp.float32)
                wanted = (ids[:, 0:1] * 256.0 + ids[:, 1:2]).astype(jnp.int32)
                wanted = wanted - scalars[4 + b]
                top = jnp.max(logits, axis=1, keepdims=True)
                if not fresh:
                    old = stats[here, :]
                    top = jnp.maximum(top, old[:, 0:1])
                mass = jnp.sum(jnp.exp(logits - top), axis=1, keepdims=True)
                found = jnp.sum(
                    jnp.where(column == wanted, logits, 0.0), axis=1, keepdims=True
                )
                if not fresh:
                    mass = mass + old[:, 1:2] * jnp.exp(old[:, 0:1] - top)
                    found = found + old[:, 2:3]
                stats[here, :] = jnp.where(
                    lane == 0, top, jnp.where(lane == 1, mass, found)
                )
                return carry

            lax.fori_loop(0, total // tile, step, 0)
    if out.shape[0] == total:
        out[...] = stats[...]
    else:
        for k in range(prev_rows // unit):
            out[scalars[6 + k]] = prev[k * unit : (k + 1) * unit, :]
        for k in range(total // unit):
            out[scalars[6 + prev_rows // unit + k]] = stats[k * unit : (k + 1) * unit, :]


def stat_call(name, scalars, hidden, weights, prev, out_units, unit, tile):
    rows = tuple(p.shape[0] for p in hidden)
    total = sum(rows)
    blocks = len(weights)
    quarter = weights[0][0].shape[0]
    prev_rows = 0 if prev is None else prev.shape[0]
    if out_units:
        out_shape = jax.ShapeDtypeStruct((out_units, unit, LANES), jnp.float32)
    else:
        out_shape = jax.ShapeDtypeStruct((total, LANES), jnp.float32)
    any_space = pl.BlockSpec(memory_space=pl.ANY)
    vmem = pl.BlockSpec(memory_space=pltpu.VMEM)
    operands = [*hidden, *(w for block in weights for w in block)]
    specs = [pl.BlockSpec(memory_space=pltpu.SMEM)] + [any_space] * len(operands)
    if prev is not None:
        operands.append(prev)
        specs.append(vmem)
    return pl.pallas_call(
        functools.partial(stat_kernel, rows, blocks, tile, prev_rows, unit),
        out_shape=out_shape,
        in_specs=specs,
        out_specs=vmem,
        scratch_shapes=[
            pltpu.VMEM((4, total, quarter), jnp.bfloat16),
            pltpu.VMEM((total, LANES), jnp.bfloat16),
            pltpu.VMEM((blocks, 4, quarter, HALF), jnp.bfloat16),
            pltpu.VMEM((total, HALF), jnp.float32),
            pltpu.VMEM((total, LANES), jnp.float32),
            pltpu.SemaphoreType.DMA((4, len(rows))),
            pltpu.SemaphoreType.DMA((len(rows),)),
            pltpu.SemaphoreType.DMA((4 * blocks,)),
        ],
        name=name,
        cost_estimate=pl.CostEstimate(
            flops=2 * total * 4 * quarter * HALF * blocks,
            bytes_accessed=2 * 4 * quarter * (total + HALF * blocks),
            transcendentals=total * HALF * blocks,
        ),
        compiler_params=pltpu.CompilerParams(vmem_limit_bytes=56 * MIB),
    )(scalars, *operands)


def merge(stats, axis):
    top = jnp.max(stats[0], axis=axis, keepdims=True)
    mass = jnp.sum(stats[1] * jnp.exp(stats[0] - top), axis=axis)
    return jnp.squeeze(top, axis), mass, jnp.sum(stats[2], axis=axis)


def local(hidden, head, targets):
    unit, depth = hidden.shape
    side, block, core = lax.axis_index("yh"), lax.axis_index("yl"), lax.axis_index("c")
    iz, ix = lax.axis_index("z"), lax.axis_index("x")
    ids = jnp.stack([targets // 256, targets % 256], axis=1).astype(jnp.bfloat16)
    u = jnp.concatenate([hidden, jnp.pad(ids, ((0, 0), (0, LANES - 2)))], axis=1)
    par = cross(u)
    quarter = head.shape[0]
    mine = lax.dynamic_slice(head, (0, HALF * side), (quarter, HALF))
    theirs = lax.dynamic_slice(head, (0, HALF * (1 - side)), (quarter, HALF))

    w_near = swap(mine, "yl")
    w_far = cross(theirs)
    w_far_own = swap(w_far, "yl")
    own_block = [mine, swap(mine, "c"), w_far_own, swap(w_far_own, "c")]
    other_block = [w_near, swap(w_near, "c"), w_far, swap(w_far, "c")]

    xm, xp = shift(u, "x", 1), shift(u, "x", -1)
    zm_u, zp_u = shift(u, "z", 1), shift(u, "z", -1)
    cut = unit // 2
    x2 = [shift(xm[:cut], "x", 1), shift(xp[cut:], "x", -1)]
    pzm, pzp = shift(par, "z", 1), shift(par, "z", -1)
    xm_par, xp_par = shift(par, "x", 1), shift(par, "x", -1)
    pz2 = [shift(pzm[:cut], "z", 1), shift(pzp[cut:], "z", -1)]
    xx, pp = jnp.concatenate([xm, xp]), jnp.concatenate([pzm, pzp])
    zm_xx, zp_xx = shift(xx, "z", 1), shift(xx, "z", -1)
    xm_pp, xp_pp = shift(pp, "x", 1), shift(pp, "x", -1)
    x2, pz2 = jnp.concatenate(x2), jnp.concatenate(pz2)
    zm_x2, zp_x2 = shift(x2, "z", 1), shift(x2, "z", -1)
    xm_pz2, xp_pz2 = shift(pz2, "x", 1), shift(pz2, "x", -1)
    z2_u, x2_par = shift(zp_u, "z", -1), shift(xp_par, "x", -1)
    z2_x2, x2_pz2 = shift(zp_x2, "z", -1), shift(xp_pz2, "x", -1)
    z2_xx, x2_pp = shift(zm_xx, "z", 1), shift(xm_pp, "x", 1)

    early = [
        (u, [(0, 0, 0)]), (xx, [(0, -1, 0), (0, 1, 0)]), (x2, [(0, 2, 0)]),
        (zm_u, [(-1, 0, 0)]), (zm_xx, [(-1, -1, 0), (-1, 1, 0)]), (zm_x2, [(-1, 2, 0)]),
        (zp_u, [(1, 0, 0)]), (zp_xx, [(1, -1, 0), (1, 1, 0)]), (zp_x2, [(1, 2, 0)]),
        (par, [(0, 0, 1)]), (pp, [(-1, 0, 1), (1, 0, 1)]), (pz2, [(2, 0, 1)]),
        (xm_par, [(0, -1, 1)]), (xm_pp, [(-1, -1, 1), (1, -1, 1)]), (xm_pz2, [(2, -1, 1)]),
        (xp_par, [(0, 1, 1)]), (xp_pp, [(-1, 1, 1), (1, 1, 1)]), (xp_pz2, [(2, 1, 1)]),
    ]
    late = [
        (z2_u, [(2, 0, 0)]), (z2_x2, [(2, 2, 0)]), (x2_par, [(0, 2, 1)]), (x2_pz2, [(2, 2, 1)]),
        (z2_xx, [(2, -1, 0), (2, 1, 0)]), (x2_pp, [(-1, 2, 1), (1, 2, 1)]),
    ]
    places = jnp.array([p for _, at in early + late for p in at], jnp.int32)
    slots = ((iz + places[:, 0]) % 4 * 4 + (ix + places[:, 1]) % 4) * 2 + places[:, 2]
    rank = jnp.array([[0, 0], [0, 1], [1, 0], [1, 1]], jnp.int32)
    quarters = (side + rank[:, 0]) % 2 * 2 + (core + rank[:, 1]) % 2
    base = (iz * 4 + ix) * 2 * 2 * HALF + HALF * side
    own_at, other_at = base + 2 * HALF * block, base + 2 * HALF * (1 - block)

    def scalars(*offsets):
        offsets = (*offsets, *offsets)[:2]
        return jnp.concatenate([quarters, jnp.stack(offsets), slots]).astype(jnp.int32)

    first = [piece for piece, _ in early]
    last = [piece for piece, _ in late]
    done = stat_call("near", scalars(other_at), first, [other_block], None, 0, unit, 384)
    done = stat_call("far", scalars(own_at), first, [own_block], done, 0, unit, 384)
    stats = stat_call(
        "late", scalars(other_at, own_at), last, [other_block, own_block], done, 32, unit, 384
    )
    stats = stats[:, :, :3].reshape(16, 2, unit, 3).transpose(0, 3, 1, 2).reshape(16, 6 * unit)
    stats = lax.all_to_all(stats, ("z", "x"), 0, 0, tiled=True).reshape(16, 3, 2, unit)
    stats = jnp.stack(merge([stats[:, k] for k in range(3)], 0))
    theirs = cross(stats[:, 1])
    top, mass, found = merge(jnp.stack([stats[:, 0], theirs], axis=1), 0)
    return found - (top + jnp.log(mass))


def solution(mesh):
    finer = Mesh(mesh.devices.reshape(4, 4, 2, 2, 2), AXES)
    placed = (P(AXES, None), P(("yh", "c"), ("z", "x", "yl")), P(AXES))
    return jax.shard_map(
        local, mesh=finer, in_specs=placed, out_specs=P(AXES), check_vma=False
    )
```

```python
import functools

import jax
import jax.numpy as jnp
from jax import lax
from jax.experimental import pallas as pl
from jax.experimental.pallas import tpu as pltpu
from jax.sharding import Mesh
from jax.sharding import PartitionSpec as P


AXES = ("z", "x", "yl", "yh", "c")
LANES = 128
HALF = 512
MIB = 2**20


def shift(x, axis, step):
    count = lax.axis_size(axis)
    return lax.ppermute(x, axis, [(k, (k + step) % count) for k in range(count)])


def swap(x, axis):
    return lax.ppermute(x, axis, [(0, 1), (1, 0)])


def cross(x):
    return lax.ppermute(x, ("yl", "yh"), [(0, 3), (3, 0), (1, 2), (2, 1)])


def stat_kernel(rows, spans, tile, prev_rows, unit, chunks, ahead, *refs):
    pieces, blocks = len(rows), len(spans)
    scalars = refs[0]
    hidden = refs[1 : 1 + pieces]
    weights = refs[1 + pieces : 1 + pieces + 4 * blocks]
    at = 1 + pieces + 4 * blocks
    prev = None
    if prev_rows:
        prev, at = refs[at], at + 1
    out, hv, tv, wv, acc, stats, hsem, tsem, wsem = refs[at:]
    total = sum(rows)
    quarter = wv.shape[1] // 4
    starts = [sum(rows[:k]) for k in range(pieces + 1)]
    steps, seen = [], set()
    for b, span in enumerate(spans):
        fresh = [k for k in range(*span) if k not in seen]
        seen.update(fresh)
        for chunk in chunks:
            copies = []
            for q in chunk:
                here = pl.ds(q * quarter, quarter)
                copies.append(
                    pltpu.make_async_copy(
                        weights[4 * b + q], wv.at[b, here, :], wsem.at[4 * b + q]
                    )
                )
                off = pl.multiple_of(scalars[q] * quarter, LANES)
                for k in fresh:
                    copies.append(
                        pltpu.make_async_copy(
                            hidden[k].at[:, pl.ds(off, quarter)],
                            hv.at[pl.ds(starts[k], rows[k]), here],
                            hsem.at[q, k],
                        )
                    )
            if chunk is chunks[-1]:
                for k in fresh:
                    copies.append(
                        pltpu.make_async_copy(
                            hidden[k].at[:, pl.ds(4 * quarter, LANES)],
                            tv.at[pl.ds(starts[k], rows[k]), :],
                            tsem.at[k],
                        )
                    )
            steps.append((b, chunk, copies))
    for n in range(min(ahead, len(steps))):
        for copy in steps[n][2]:
            copy.start()
    lane = lax.broadcasted_iota(jnp.int32, (tile, LANES), 1)
    column = lax.broadcasted_iota(jnp.int32, (tile, HALF), 1)
    carried = out.shape[0] == total
    known = prev_rows if carried else 0
    if known:
        stats[0:known, :] = prev[...]
    for n, (b, chunk, copies) in enumerate(steps):
        for copy in copies:
            copy.wait()
        if n + ahead < len(steps):
            for copy in steps[n + ahead][2]:
                copy.start()
        first, stop = starts[spans[b][0]], starts[spans[b][1]]

        def step(r, carry, b=b, chunk=chunk, first=first, merging=bool(b)):
            here = pl.ds(pl.multiple_of(first + r * tile, 48), tile)
            deep = slice(chunk[0] * quarter, (chunk[-1] + 1) * quarter)
            part = jnp.dot(
                hv[here, deep], wv[b, deep, :], preferred_element_type=jnp.float32
            )
            if chunk is not chunks[0]:
                part = acc[here, :] + part
            if chunk is not chunks[-1]:
                acc[here, :] = part
                return carry
            ids = tv[here, :].astype(jnp.float32)
            wanted = (ids[:, 0:1] * 256.0 + ids[:, 1:2]).astype(jnp.int32)
            wanted = wanted - scalars[4 + b]
            top = jnp.max(part, axis=1, keepdims=True)
            if merging:
                old = stats[here, :]
                top = jnp.maximum(top, old[:, 0:1])
            mass = jnp.sum(jnp.exp(part - top), axis=1, keepdims=True)
            found = jnp.sum(
                jnp.where(column == wanted, part, 0.0), axis=1, keepdims=True
            )
            if merging:
                mass = mass + old[:, 1:2] * jnp.exp(old[:, 0:1] - top)
                found = found + old[:, 2:3]
            stats[here, :] = jnp.where(
                lane == 0, top, jnp.where(lane == 1, mass, found)
            )
            return carry

        lax.fori_loop(0, (stop - first) // tile, step, 0)
    if carried:
        out[...] = stats[...]
    else:
        for k in range(prev_rows // unit):
            out[scalars[6 + k]] = prev[k * unit : (k + 1) * unit, :]
        for k in range(total // unit):
            out[scalars[6 + prev_rows // unit + k]] = stats[k * unit : (k + 1) * unit, :]


def stat_call(scalars, hidden, weights, spans, prev, out_units, unit, tile, chunks, ahead):
    rows = tuple(p.shape[0] for p in hidden)
    total = sum(rows)
    blocks = len(weights)
    quarter = weights[0][0].shape[0]
    prev_rows = 0 if prev is None else prev.shape[0]
    if out_units:
        out_shape = jax.ShapeDtypeStruct((out_units, unit, LANES), jnp.float32)
    else:
        out_shape = jax.ShapeDtypeStruct((total, LANES), jnp.float32)
    any_space = pl.BlockSpec(memory_space=pl.ANY)
    vmem = pl.BlockSpec(memory_space=pltpu.VMEM)
    operands = [*hidden, *(w for block in weights for w in block)]
    specs = [pl.BlockSpec(memory_space=pltpu.SMEM)] + [any_space] * len(operands)
    if prev is not None:
        operands.append(prev)
        specs.append(vmem)
    return pl.pallas_call(
        functools.partial(stat_kernel, rows, spans, tile, prev_rows, unit, chunks, ahead),
        out_shape=out_shape,
        in_specs=specs,
        out_specs=vmem,
        scratch_shapes=[
            pltpu.VMEM((total, 4 * quarter), jnp.bfloat16),
            pltpu.VMEM((total, LANES), jnp.bfloat16),
            pltpu.VMEM((blocks, 4 * quarter, HALF), jnp.bfloat16),
            pltpu.VMEM((total, HALF), jnp.float32),
            pltpu.VMEM((total, LANES), jnp.float32),
            pltpu.SemaphoreType.DMA((4, len(rows))),
            pltpu.SemaphoreType.DMA((len(rows),)),
            pltpu.SemaphoreType.DMA((4 * blocks,)),
        ],
        cost_estimate=pl.CostEstimate(
            flops=2 * total * 4 * quarter * HALF * blocks,
            bytes_accessed=2 * 4 * quarter * (total + HALF * blocks),
            transcendentals=total * HALF * blocks,
        ),
        compiler_params=pltpu.CompilerParams(vmem_limit_bytes=56 * MIB),
    )(scalars, *operands)


def merge(stats, axis):
    top = jnp.max(stats[0], axis=axis, keepdims=True)
    mass = jnp.sum(stats[1] * jnp.exp(stats[0] - top), axis=axis)
    return jnp.squeeze(top, axis), mass, jnp.sum(stats[2], axis=axis)


def local(hidden, head, targets):
    unit, _ = hidden.shape
    side, block, core = lax.axis_index("yh"), lax.axis_index("yl"), lax.axis_index("c")
    iz, ix = lax.axis_index("z"), lax.axis_index("x")
    ids = jnp.stack([targets // 256, targets % 256], axis=1).astype(jnp.bfloat16)
    u = jnp.concatenate([hidden, jnp.pad(ids, ((0, 0), (0, LANES - 2)))], axis=1)
    quarter = head.shape[0]
    mine = lax.dynamic_slice(head, (0, HALF * side), (quarter, HALF))
    theirs = lax.dynamic_slice(head, (0, HALF * (1 - side)), (quarter, HALF))
    cut = unit // 2

    par = cross(u)
    xm, xp = shift(u, "x", 1), shift(u, "x", -1)
    zm_u, zp_u = shift(u, "z", 1), shift(u, "z", -1)
    w_near = swap(mine, "yl")
    w_far = cross(theirs)
    w_mine_c = swap(mine, "c")

    pzm, pzp = shift(par, "z", 1), shift(par, "z", -1)
    x2 = [shift(xm[:cut], "x", 1), shift(xp[cut:], "x", -1)]
    xm_par, xp_par = shift(par, "x", 1), shift(par, "x", -1)
    zm_xm, zp_xm = shift(xm, "z", 1), shift(xm, "z", -1)

    pz2 = [shift(pzm[:cut], "z", 1), shift(pzp[cut:], "z", -1)]
    pp = jnp.concatenate([pzm, pzp])
    xm_pp, xp_pp = shift(pp, "x", 1), shift(pp, "x", -1)
    zm_xp, zp_xp = shift(xp, "z", 1), shift(xp, "z", -1)
    x2, pz2 = jnp.concatenate(x2), jnp.concatenate(pz2)
    zm_x2, zp_x2 = shift(x2, "z", 1), shift(x2, "z", -1)
    z2_u = shift(zp_u, "z", -1)
    xm_pz2, xp_pz2 = shift(pz2, "x", 1), shift(pz2, "x", -1)
    x2_par = shift(xp_par, "x", -1)

    w_near_c = swap(w_near, "c")
    w_far_own = swap(w_far, "yl")
    w_far_c = swap(w_far, "c")
    z2_xm, z2_xp = shift(zm_xm, "z", 1), shift(zm_xp, "z", 1)
    x2_pp = shift(xm_pp, "x", 1)
    z2_x2, x2_pz2 = shift(zp_x2, "z", -1), shift(xp_pz2, "x", -1)
    w_far_own_c = swap(w_far_own, "c")
    own_block = [mine, w_mine_c, w_far_own, w_far_own_c]
    other_block = [w_near, w_near_c, w_far, w_far_c]

    early = [
        (u, [(0, 0, 0)]), (xm, [(0, -1, 0)]), (xp, [(0, 1, 0)]), (x2, [(0, 2, 0)]),
        (zm_u, [(-1, 0, 0)]), (zp_u, [(1, 0, 0)]),
        (par, [(0, 0, 1)]), (pp, [(-1, 0, 1), (1, 0, 1)]), (pz2, [(2, 0, 1)]),
        (xm_par, [(0, -1, 1)]), (xp_par, [(0, 1, 1)]),
    ]
    middle = [
        (zm_xm, [(-1, -1, 0)]), (zm_xp, [(-1, 1, 0)]), (zm_x2, [(-1, 2, 0)]),
        (zp_xm, [(1, -1, 0)]), (zp_xp, [(1, 1, 0)]), (zp_x2, [(1, 2, 0)]),
        (xm_pp, [(-1, -1, 1), (1, -1, 1)]), (xm_pz2, [(2, -1, 1)]),
        (xp_pp, [(-1, 1, 1), (1, 1, 1)]), (xp_pz2, [(2, 1, 1)]),
    ]
    late = [
        (z2_u, [(2, 0, 0)]), (z2_x2, [(2, 2, 0)]), (x2_par, [(0, 2, 1)]), (x2_pz2, [(2, 2, 1)]),
        (z2_xm, [(2, -1, 0)]), (z2_xp, [(2, 1, 0)]), (x2_pp, [(-1, 2, 1), (1, 2, 1)]),
    ]
    places = jnp.array([p for _, at in early + middle + late for p in at], jnp.int32)
    slots = ((iz + places[:, 0]) % 4 * 4 + (ix + places[:, 1]) % 4) * 2 + places[:, 2]
    rank = jnp.array([[0, 0], [0, 1], [1, 0], [1, 1]], jnp.int32)
    quarters = (side + rank[:, 0]) % 2 * 2 + (core + rank[:, 1]) % 2
    base = (iz * 4 + ix) * 2 * 2 * HALF + HALF * side
    own_at, other_at = base + 2 * HALF * block, base + 2 * HALF * (1 - block)

    def scalars(*offsets):
        offsets = (*offsets, *offsets)[:2]
        return jnp.concatenate([quarters, jnp.stack(offsets), slots]).astype(jnp.int32)

    first, second, third = ([piece for piece, _ in group] for group in (early, middle, late))
    pair, each = ((0, 1), (2, 3)), ((0,), (1,), (2,), (3,))
    one, all_ = len(first), len(first) + len(second)
    at = scalars(other_at)
    done = stat_call(at, first, [other_block], [(0, one)], None, 0, unit, 576, each, 2)
    both, at = [other_block, own_block], scalars(other_at, own_at)
    done = stat_call(
        at, first + second, both, [(one, all_), (0, all_)], done, 0, unit, 576, pair, 1
    )
    spans = [(0, len(third))] * 2
    stats = stat_call(at, third, both, spans, done, 32, unit, 384, each, 3)
    stats = stats[:, :, :3].reshape(16, 2, unit, 3).transpose(0, 3, 1, 2).reshape(16, 6 * unit)
    stats = lax.all_to_all(stats, ("z", "x"), 0, 0, tiled=True).reshape(16, 3, 2, unit)
    stats = jnp.stack(merge([stats[:, k] for k in range(3)], 0))
    theirs = cross(stats[:, 1])
    top, mass, found = merge(jnp.stack([stats[:, 0], theirs], axis=1), 0)
    return found - (top + jnp.log(mass))


def solution(mesh):
    finer = Mesh(mesh.devices.reshape(4, 4, 2, 2, 2), AXES)
    placed = (P(AXES, None), P(("yh", "c"), ("z", "x", "yl")), P(AXES))
    return jax.shard_map(local, mesh=finer, in_specs=placed, out_specs=P(AXES), check_vma=False)
```

```python
import functools

import jax
import jax.numpy as jnp
from jax import lax
from jax.experimental import pallas as pl
from jax.experimental.pallas import tpu as pltpu
from jax.sharding import Mesh
from jax.sharding import PartitionSpec as P


AXES = ("z", "x", "yl", "yh", "c")
LANES = 128
HALF = 512
MIB = 2**20


def shift(x, axis, step):
    count = lax.axis_size(axis)
    return lax.ppermute(x, axis, [(k, (k + step) % count) for k in range(count)])


def swap(x, axis):
    return lax.ppermute(x, axis, [(0, 1), (1, 0)])


def cross(x):
    return lax.ppermute(x, ("yl", "yh"), [(0, 3), (3, 0), (1, 2), (2, 1)])


def stat_kernel(rows, parts, tile, prev_rows, unit, chunks, ahead, *refs):
    pieces, count = len(rows), len([n for block in parts for some in block for n in some])
    scalars = refs[0]
    hidden = refs[1 : 1 + pieces]
    weights = list(refs[1 + pieces : 1 + pieces + count])
    prevs = refs[1 + pieces + count : 1 + pieces + count + len(prev_rows)]
    out, hv, tv, wv, acc, stats, hsem, tsem, wsem = refs[1 + pieces + count + len(prev_rows) :]
    total, quarter = sum(rows), wv.shape[0] // 4
    starts = [sum(rows[:k]) for k in range(pieces)]
    loads, n = {q: [] for q in range(4)}, 0
    for b, block in enumerate(parts):
        for q, some in enumerate(block):
            at = q * quarter
            for length in some:
                place = wv.at[pl.ds(at, length), pl.ds(b * HALF, HALF)]
                loads[q].append(pltpu.make_async_copy(weights[n], place, wsem.at[n]))
                at, n = at + length, n + 1
    for q in range(4):
        off = pl.multiple_of(scalars[q] * quarter, LANES)
        for k in range(pieces):
            place = hv.at[pl.ds(starts[k], rows[k]), pl.ds(q * quarter, quarter)]
            source = hidden[k].at[:, pl.ds(off, quarter)]
            loads[q].append(pltpu.make_async_copy(source, place, hsem.at[q, k]))
    for k in range(pieces):
        place = tv.at[pl.ds(starts[k], rows[k]), :]
        source = hidden[k].at[:, pl.ds(4 * quarter, LANES)]
        loads[3].append(pltpu.make_async_copy(source, place, tsem.at[k]))
    steps = [[copy for q in chunk for copy in loads[q]] for chunk in chunks]
    for copies in steps[:ahead]:
        for copy in copies:
            copy.start()
    lane = lax.broadcasted_iota(jnp.int32, (tile, LANES), 1)
    column = lax.broadcasted_iota(jnp.int32, (tile, 2 * HALF), 1)
    column = column + jnp.where(column < HALF, scalars[4], scalars[5] - HALF)
    for n, chunk in enumerate(chunks):
        for copy in steps[n]:
            copy.wait()
        if n + ahead < len(steps):
            for copy in steps[n + ahead]:
                copy.start()

        def step(r, carry, n=n, chunk=chunk):
            here = pl.ds(pl.multiple_of(r * tile, tile), tile)
            deep = slice(chunk[0] * quarter, (chunk[-1] + 1) * quarter)
            part = jnp.dot(hv[here, deep], wv[deep, :], preferred_element_type=jnp.float32)
            if n:
                part = acc[here, :] + part
            if n + 1 < len(chunks):
                acc[here, :] = part
                return carry
            ids = tv[here, :].astype(jnp.float32)
            wanted = (ids[:, 0:1] * 256.0 + ids[:, 1:2]).astype(jnp.int32)
            top = jnp.max(part, axis=1, keepdims=True)
            mass = jnp.sum(jnp.exp(part - top), axis=1, keepdims=True)
            found = jnp.sum(jnp.where(column == wanted, part, 0.0), axis=1, keepdims=True)
            stats[here, :] = jnp.where(lane == 0, top, jnp.where(lane == 1, mass, found))
            return carry

        lax.fori_loop(0, total // tile, step, 0)
    if not prev_rows:
        out[...] = stats[...]
        return
    at = 0
    for source, length in [*zip(prevs, prev_rows), (stats, total)]:
        for k in range(length // unit):
            out[scalars[6 + at]] = source[k * unit : (k + 1) * unit, :]
            at += 1


def stat_call(scalars, hidden, weights, prevs, out_units, unit, tile, chunks, ahead):
    rows = tuple(p.shape[0] for p in hidden)
    total = sum(rows)
    parts = tuple(tuple(tuple(w.shape[0] for w in some) for some in block) for block in weights)
    depth = sum(n for some in parts[0] for n in some)
    prev_rows = tuple(p.shape[0] for p in prevs)
    if out_units:
        out_shape = jax.ShapeDtypeStruct((out_units, unit, LANES), jnp.float32)
    else:
        out_shape = jax.ShapeDtypeStruct((total, LANES), jnp.float32)
    any_space = pl.BlockSpec(memory_space=pl.ANY)
    vmem = pl.BlockSpec(memory_space=pltpu.VMEM)
    loaded = [w for block in weights for some in block for w in some]
    operands = [*hidden, *loaded]
    specs = [pl.BlockSpec(memory_space=pltpu.SMEM)] + [any_space] * len(operands)
    return pl.pallas_call(
        functools.partial(stat_kernel, rows, parts, tile, prev_rows, unit, chunks, ahead),
        out_shape=out_shape,
        in_specs=specs + [vmem] * len(prevs),
        out_specs=vmem,
        scratch_shapes=[
            pltpu.VMEM((total, depth), jnp.bfloat16),
            pltpu.VMEM((total, LANES), jnp.bfloat16),
            pltpu.VMEM((depth, 2 * HALF), jnp.bfloat16),
            pltpu.VMEM((total, 2 * HALF), jnp.float32),
            pltpu.VMEM((total, LANES), jnp.float32),
            pltpu.SemaphoreType.DMA((4, len(rows))),
            pltpu.SemaphoreType.DMA((len(rows),)),
            pltpu.SemaphoreType.DMA((len(loaded),)),
        ],
        cost_estimate=pl.CostEstimate(
            flops=4 * total * depth * HALF,
            bytes_accessed=2 * depth * (total + 2 * HALF),
            transcendentals=2 * total * HALF,
        ),
        compiler_params=pltpu.CompilerParams(vmem_limit_bytes=56 * MIB),
    )(scalars, *operands, *prevs)


def merge(stats, axis):
    top = jnp.max(stats[0], axis=axis, keepdims=True)
    mass = jnp.sum(stats[1] * jnp.exp(stats[0] - top), axis=axis)
    return jnp.squeeze(top, axis), mass, jnp.sum(stats[2], axis=axis)


def local(hidden, head, targets):
    unit, _ = hidden.shape
    side, block, core = lax.axis_index("yh"), lax.axis_index("yl"), lax.axis_index("c")
    iz, ix = lax.axis_index("z"), lax.axis_index("x")
    ids = jnp.stack([targets // 256, targets % 256], axis=1).astype(jnp.bfloat16)
    u = jnp.concatenate([hidden, jnp.pad(ids, ((0, 0), (0, LANES - 2)))], axis=1)
    quarter = head.shape[0]
    mine = lax.dynamic_slice(head, (0, HALF * side), (quarter, HALF))
    theirs = lax.dynamic_slice(head, (0, HALF * (1 - side)), (quarter, HALF))
    cut = unit // 2

    par = cross(u)
    xm, xp = shift(u, "x", 1), shift(u, "x", -1)
    zm_u, zp_u = shift(u, "z", 1), shift(u, "z", -1)
    w_near = swap(mine, "yl")
    low, high = theirs[: quarter // 2], theirs[quarter // 2 :]
    w_far = [cross(low), cross(high)]
    w_mine_c = swap(mine, "c")

    pzm, pzp = shift(par, "z", 1), shift(par, "z", -1)
    x2 = [shift(xm[:cut], "x", 1), shift(xp[cut:], "x", -1)]
    xm_par, xp_par = shift(par, "x", 1), shift(par, "x", -1)
    zm_xm, zp_xm = shift(xm, "z", 1), shift(xm, "z", -1)

    pz2 = [shift(pzm[:cut], "z", 1), shift(pzp[cut:], "z", -1)]
    pp = jnp.concatenate([pzm, pzp])
    xm_pp, xp_pp = shift(pp, "x", 1), shift(pp, "x", -1)
    zm_xp, zp_xp = shift(xp, "z", 1), shift(xp, "z", -1)
    x2, pz2 = jnp.concatenate(x2), jnp.concatenate(pz2)
    zm_x2, zp_x2 = shift(x2, "z", 1), shift(x2, "z", -1)
    z2_u = shift(zp_u, "z", -1)
    xm_pz2, xp_pz2 = shift(pz2, "x", 1), shift(pz2, "x", -1)
    x2_par = shift(xp_par, "x", -1)

    w_near_c = swap(w_near, "c")
    w_far_own = [swap(w_far[0], "yl"), swap(w_far[1], "yl")]
    w_far_c = [swap(w_far[0], "c"), swap(w_far[1], "c")]
    z2_xm, z2_xp = shift(zm_xm, "z", 1), shift(zm_xp, "z", 1)
    x2_pp = shift(xm_pp, "x", 1)
    z2_x2, x2_pz2 = shift(zp_x2, "z", -1), shift(xp_pz2, "x", -1)
    w_own_c = [swap(w_far_own[0], "c"), swap(w_far_own[1], "c")]
    own_block = [[mine], [w_mine_c], w_far_own, w_own_c]
    other_block = [[w_near], [w_near_c], w_far, w_far_c]

    early = [
        (u, [(0, 0, 0)]), (xm, [(0, -1, 0)]), (xp, [(0, 1, 0)]), (x2, [(0, 2, 0)]),
        (zm_u, [(-1, 0, 0)]), (zp_u, [(1, 0, 0)]),
        (par, [(0, 0, 1)]), (pp, [(-1, 0, 1), (1, 0, 1)]), (pz2, [(2, 0, 1)]),
        (xm_par, [(0, -1, 1)]), (xp_par, [(0, 1, 1)]),
    ]
    middle = [
        (zm_xm, [(-1, -1, 0)]), (zm_xp, [(-1, 1, 0)]), (zm_x2, [(-1, 2, 0)]),
        (zp_xm, [(1, -1, 0)]), (zp_xp, [(1, 1, 0)]), (zp_x2, [(1, 2, 0)]),
        (xm_pp, [(-1, -1, 1), (1, -1, 1)]), (xm_pz2, [(2, -1, 1)]),
        (xp_pp, [(-1, 1, 1), (1, 1, 1)]), (xp_pz2, [(2, 1, 1)]),
    ]
    late = [
        (z2_u, [(2, 0, 0)]), (z2_x2, [(2, 2, 0)]), (x2_par, [(0, 2, 1)]), (x2_pz2, [(2, 2, 1)]),
        (z2_xm, [(2, -1, 0)]), (z2_xp, [(2, 1, 0)]), (x2_pp, [(-1, 2, 1), (1, 2, 1)]),
    ]
    places = jnp.array([p for _, at in early + middle + late for p in at], jnp.int32)
    slots = ((iz + places[:, 0]) % 4 * 4 + (ix + places[:, 1]) % 4) * 2 + places[:, 2]
    rank = jnp.array([[0, 0], [0, 1], [1, 0], [1, 1]], jnp.int32)
    quarters = (side + rank[:, 0]) % 2 * 2 + (core + rank[:, 1]) % 2
    base = (iz * 4 + ix) * 2 * 2 * HALF + HALF * side
    own_at, other_at = base + 2 * HALF * block, base + 2 * HALF * (1 - block)

    at = jnp.concatenate([quarters, jnp.stack([other_at, own_at]), slots]).astype(jnp.int32)
    first, second, third = ([piece for piece, _ in group] for group in (early, middle, late))
    weights, each = [other_block, own_block], ((0,), (1,), (2,), (3,))
    near = stat_call(at, first, weights, [], 0, unit, 576, each, 2)
    far = stat_call(at, second, weights, [], 0, unit, 576, each, 2)
    stats = stat_call(at, third, weights, [near, far], 32, unit, 384, each, 3)
    stats = stats[:, :, :3].reshape(16, 2, unit, 3).transpose(0, 3, 1, 2).reshape(16, 6 * unit)
    stats = lax.all_to_all(stats, ("z", "x"), 0, 0, tiled=True).reshape(16, 3, 2, unit)
    stats = jnp.stack(merge([stats[:, k] for k in range(3)], 0))
    theirs = cross(stats[:, 1])
    top, mass, found = merge(jnp.stack([stats[:, 0], theirs], axis=1), 0)
    return found - (top + jnp.log(mass))


def solution(mesh):
    finer = Mesh(mesh.devices.reshape(4, 4, 2, 2, 2), AXES)
    placed = (P(AXES, None), P(("yh", "c"), ("z", "x", "yl")), P(AXES))
    return jax.shard_map(local, mesh=finer, in_specs=placed, out_specs=P(AXES), check_vma=False)
```

```python
import functools

import jax
import jax.numpy as jnp
from jax import lax
from jax.experimental import pallas as pl
from jax.experimental.pallas import tpu as pltpu
from jax.sharding import Mesh
from jax.sharding import PartitionSpec as P


AXES = ("z", "x", "yl", "yh", "c")
LANES = 128
HALF = 512
MIB = 2**20


PEERS = [[2 * k + (k + odd) % 2 for k in range(32)] for odd in (0, 1)]


def shift(x, axis, step):
    count = lax.axis_size(axis)
    return lax.ppermute(x, axis, [(k, (k + step) % count) for k in range(count)])


def swap(x, axis):
    return lax.ppermute(x, axis, [(0, 1), (1, 0)])


def cross(x):
    return lax.ppermute(x, ("yl", "yh"), [(0, 3), (3, 0), (1, 2), (2, 1)])


def stat_kernel(rows, parts, tile, prev_units, unit, chunks, ahead, *refs):
    pieces, count = len(rows), len([n for block in parts for some in block for n in some])
    scalars = refs[0]
    hidden = refs[1 : 1 + pieces]
    weights = list(refs[1 + pieces : 1 + pieces + count])
    prevs = refs[1 + pieces + count : 1 + pieces + count + len(prev_units)]
    out, hv, tv, wv, acc, stats, hsem, tsem, wsem = refs[1 + pieces + count + len(prev_units) :]
    total, quarter = sum(rows), wv.shape[0] // 4
    starts = [sum(rows[:k]) for k in range(pieces)]
    loads, n = {q: [] for q in range(4)}, 0
    for b, block in enumerate(parts):
        for q, some in enumerate(block):
            at = q * quarter
            for length in some:
                place = wv.at[pl.ds(at, length), pl.ds(b * HALF, HALF)]
                loads[q].append(pltpu.make_async_copy(weights[n], place, wsem.at[n]))
                at, n = at + length, n + 1
    for q in range(4):
        off = pl.multiple_of(scalars[q] * quarter, LANES)
        for k in range(pieces):
            place = hv.at[pl.ds(starts[k], rows[k]), pl.ds(q * quarter, quarter)]
            source = hidden[k].at[:, pl.ds(off, quarter)]
            loads[q].append(pltpu.make_async_copy(source, place, hsem.at[q, k]))
    for k in range(pieces):
        place = tv.at[pl.ds(starts[k], rows[k]), :]
        source = hidden[k].at[:, pl.ds(4 * quarter, LANES)]
        loads[3].append(pltpu.make_async_copy(source, place, tsem.at[k]))
    steps = [[copy for q in chunk for copy in loads[q]] for chunk in chunks]
    for copies in steps[:ahead]:
        for copy in copies:
            copy.start()
    lane = lax.broadcasted_iota(jnp.int32, (tile, LANES), 1)
    column = lax.broadcasted_iota(jnp.int32, (tile, 2 * HALF), 1)
    column = column + jnp.where(column < HALF, scalars[4], scalars[5] - HALF)
    for n, chunk in enumerate(chunks):
        for copy in steps[n]:
            copy.wait()
        if n + ahead < len(steps):
            for copy in steps[n + ahead]:
                copy.start()

        def step(r, carry, n=n, chunk=chunk):
            here = pl.ds(pl.multiple_of(r * tile, tile), tile)
            deep = slice(chunk[0] * quarter, (chunk[-1] + 1) * quarter)
            part = jnp.dot(hv[here, deep], wv[deep, :], preferred_element_type=jnp.float32)
            if n:
                part = acc[here, :] + part
            if n + 1 < len(chunks):
                acc[here, :] = part
                return carry
            ids = tv[here, :].astype(jnp.float32)
            wanted = (ids[:, 0:1] * 256.0 + ids[:, 1:2]).astype(jnp.int32)
            top = jnp.max(part, axis=1, keepdims=True)
            mass = jnp.sum(jnp.exp(part - top), axis=1, keepdims=True)
            found = jnp.sum(jnp.where(column == wanted, part, 0.0), axis=1, keepdims=True)
            stats[here, :] = jnp.where(lane == 0, top, jnp.where(lane == 1, mass, found))
            return carry

        lax.fori_loop(0, total // tile, step, 0)
    done = 0
    for source, length in zip(prevs, prev_units):
        for k in range(length):
            out[scalars[6 + done]] = source[k]
            done += 1
    for k in range(total // unit):
        turned = jnp.transpose(stats[k * unit : k * unit + LANES, :])
        out[scalars[6 + done + k] if prevs else k] = turned[0:8, :]


def stat_call(scalars, hidden, weights, prevs, out_units, unit, tile, chunks, ahead):
    rows = tuple(p.shape[0] for p in hidden)
    total = sum(rows)
    parts = tuple(tuple(tuple(w.shape[0] for w in some) for some in block) for block in weights)
    depth = sum(n for some in parts[0] for n in some)
    prev_units = tuple(p.shape[0] for p in prevs)
    out_shape = jax.ShapeDtypeStruct((out_units or total // unit, 8, LANES), jnp.float32)
    any_space = pl.BlockSpec(memory_space=pl.ANY)
    vmem = pl.BlockSpec(memory_space=pltpu.VMEM)
    loaded = [w for block in weights for some in block for w in some]
    operands = [*hidden, *loaded]
    specs = [pl.BlockSpec(memory_space=pltpu.SMEM)] + [any_space] * len(operands)
    return pl.pallas_call(
        functools.partial(stat_kernel, rows, parts, tile, prev_units, unit, chunks, ahead),
        out_shape=out_shape,
        in_specs=specs + [vmem] * len(prevs),
        out_specs=vmem,
        scratch_shapes=[
            pltpu.VMEM((total, depth), jnp.bfloat16),
            pltpu.VMEM((total, LANES), jnp.bfloat16),
            pltpu.VMEM((depth, 2 * HALF), jnp.bfloat16),
            pltpu.VMEM((total, 2 * HALF), jnp.float32),
            pltpu.VMEM((total + LANES, LANES), jnp.float32),
            pltpu.SemaphoreType.DMA((4, len(rows))),
            pltpu.SemaphoreType.DMA((len(rows),)),
            pltpu.SemaphoreType.DMA((len(loaded),)),
        ],
        cost_estimate=pl.CostEstimate(
            flops=4 * total * depth * HALF,
            bytes_accessed=2 * depth * (total + 2 * HALF),
            transcendentals=2 * total * HALF,
        ),
        compiler_params=pltpu.CompilerParams(vmem_limit_bytes=56 * MIB),
    )(scalars, *operands, *prevs)


def local(hidden, head, targets):
    unit, _ = hidden.shape
    side, block, core = lax.axis_index("yh"), lax.axis_index("yl"), lax.axis_index("c")
    iz, ix = lax.axis_index("z"), lax.axis_index("x")
    ids = jnp.stack([targets // 256, targets % 256], axis=1).astype(jnp.bfloat16)
    u = jnp.concatenate([hidden, jnp.pad(ids, ((0, 0), (0, LANES - 2)))], axis=1)
    quarter = head.shape[0]
    half = quarter // 2
    mine = lax.dynamic_slice(head, (0, HALF * side), (quarter, HALF))
    low, high = (
        lax.dynamic_slice(head, (at, HALF * (1 - side)), (half, HALF)) for at in (0, half)
    )
    cut = unit // 2

    par = cross(u)
    xm, xp = shift(u, "x", 1), shift(u, "x", -1)
    zm_u, zp_u = shift(u, "z", 1), shift(u, "z", -1)
    w_near = swap(mine, "yl")
    w_far = [cross(low), cross(high)]
    w_mine_c = swap(mine, "c")

    pzm, pzp = shift(par, "z", 1), shift(par, "z", -1)
    x2 = [shift(xm[:cut], "x", 1), shift(xp[cut:], "x", -1)]
    xm_par, xp_par = shift(par, "x", 1), shift(par, "x", -1)
    zm_xm, zp_xm = shift(xm, "z", 1), shift(xm, "z", -1)

    pz2 = [shift(pzm[:cut], "z", 1), shift(pzp[cut:], "z", -1)]
    pp = jnp.concatenate([pzm, pzp])
    xm_pp, xp_pp = shift(pp, "x", 1), shift(pp, "x", -1)
    zm_xp, zp_xp = shift(xp, "z", 1), shift(xp, "z", -1)
    x2, pz2 = jnp.concatenate(x2), jnp.concatenate(pz2)
    zm_x2, zp_x2 = shift(x2, "z", 1), shift(x2, "z", -1)
    x2_par, z2_u = cross(x2), cross(pz2)
    xm_pz2, xp_pz2 = shift(pz2, "x", 1), shift(pz2, "x", -1)

    w_near_c = swap(w_near, "c")
    w_far_own = [swap(w_far[0], "yl"), swap(w_far[1], "yl")]
    w_far_c = [swap(w_far[0], "c"), swap(w_far[1], "c")]
    z2_xm = shift(zm_xm, "z", 1)
    z2_xp = [shift(zm_xp[:32], "z", 1), shift(zp_xp[32:], "z", -1)]
    x2_pp = [shift(xm_pp[:80], "x", 1), shift(xp_pp[80:], "x", -1)]
    z2_x2, x2_pz2 = shift(zp_x2, "z", -1), shift(xp_pz2, "x", -1)
    w_own_c = [swap(w_far_own[0], "c"), swap(w_far_own[1], "c")]
    own_block = [[mine], [w_mine_c], w_far_own, w_own_c]
    other_block = [[w_near], [w_near_c], w_far, w_far_c]

    early = [
        (u, [(0, 0, 0)]), (xm, [(0, -1, 0)]), (xp, [(0, 1, 0)]), (x2, [(0, 2, 0)]),
        (zm_u, [(-1, 0, 0)]), (zp_u, [(1, 0, 0)]),
        (par, [(0, 0, 1)]), (pp, [(-1, 0, 1), (1, 0, 1)]), (pz2, [(2, 0, 1)]),
        (xm_par, [(0, -1, 1)]), (xp_par, [(0, 1, 1)]),
    ]
    middle = [
        (zm_xm, [(-1, -1, 0)]), (zm_xp, [(-1, 1, 0)]), (zm_x2, [(-1, 2, 0)]),
        (zp_xm, [(1, -1, 0)]), (zp_xp, [(1, 1, 0)]), (zp_x2, [(1, 2, 0)]),
        (xm_pp, [(-1, -1, 1), (1, -1, 1)]), (xm_pz2, [(2, -1, 1)]),
        (xp_pp, [(-1, 1, 1), (1, 1, 1)]), (xp_pz2, [(2, 1, 1)]),
    ]
    early += [(x2_par, [(0, 2, 1)])]
    middle += [(z2_u, [(2, 0, 0)])]
    late = [
        (z2_x2, [(2, 2, 0)]), (x2_pz2, [(2, 2, 1)]), (z2_xm, [(2, -1, 0)]),
        (z2_xp[0], [(2, 1, 0)]), (z2_xp[1], []),
        (x2_pp[0], [(-1, 2, 1), (1, 2, 1)]), (x2_pp[1], []),
    ]
    places = jnp.array([p for _, at in early + middle + late for p in at], jnp.int32)
    slots = (iz + places[:, 0]) % 4 * 4 + (ix + places[:, 1]) % 4
    slots = slots * 2 + (block + places[:, 2]) % 2
    rank = jnp.array([[0, 0], [0, 1], [1, 0], [1, 1]], jnp.int32)
    quarters = (side + rank[:, 0]) % 2 * 2 + (core + rank[:, 1]) % 2
    base = (iz * 4 + ix) * 2 * 2 * HALF + HALF * side
    own_at, other_at = base + 2 * HALF * block, base + 2 * HALF * (1 - block)

    at = jnp.concatenate([quarters, jnp.stack([other_at, own_at]), slots]).astype(jnp.int32)
    first, second, third = ([piece for piece, _ in group] for group in (early, middle, late))
    weights, each = [other_block, own_block], ((0,), (1,), (2,), (3,))
    near = stat_call(at, first, weights, [], 0, unit, 624, each, 2)
    far = stat_call(at, second, weights, [], 0, unit, 624, each, 2)
    stats = stat_call(at, third, weights, [near, far], 32, unit, 288, each, 3)
    stats = lax.all_to_all(
        stats, ("z", "x", "yl", "yh"), 0, 0, tiled=True, axis_index_groups=PEERS
    )
    tops, masses, found = (stats[:, k, :unit] for k in range(3))
    top = jnp.max(tops, axis=0)
    mass = jnp.sum(masses * jnp.exp(tops - top), axis=0)
    return jnp.sum(found, axis=0) - (top + jnp.log(mass))


def solution(mesh):
    finer = Mesh(mesh.devices.reshape(4, 4, 2, 2, 2), AXES)
    placed = (P(AXES, None), P(("yh", "c"), ("z", "x", "yl")), P(AXES))
    return jax.shard_map(local, mesh=finer, in_specs=placed, out_specs=P(AXES), check_vma=False)
```

```python
import functools

import jax
import jax.numpy as jnp
from jax import lax
from jax.experimental import pallas as pl
from jax.experimental.pallas import tpu as pltpu
from jax.sharding import Mesh
from jax.sharding import PartitionSpec as P


AXES = ("z", "x", "yl", "yh", "c")
LANES = 128
HALF = 512
MIB = 2**20


PEERS = [[2 * k + (k + odd) % 2 for k in range(32)] for odd in (0, 1)]


def shift(x, axis, step):
    count = lax.axis_size(axis)
    return lax.ppermute(x, axis, [(k, (k + step) % count) for k in range(count)])


def swap(x, axis):
    return lax.ppermute(x, axis, [(0, 1), (1, 0)])


def cross(x):
    return lax.ppermute(x, ("yl", "yh"), [(0, 3), (3, 0), (1, 2), (2, 1)])


def stat_kernel(rows, parts, stages, prev_units, unit, ahead, raw, *refs):
    pieces, count = len(rows), len([n for block in parts for some in block for n in some])
    scalars = refs[0]
    hidden = refs[1 : 1 + pieces]
    weights = list(refs[1 + pieces : 1 + pieces + count])
    prevs = refs[1 + pieces + count : 1 + pieces + count + len(prev_units)]
    out, hv, tv, wv, acc, stats, hsem, tsem, wsem = refs[1 + pieces + count + len(prev_units) :]
    total, quarter = sum(rows), wv.shape[0] // 4
    starts = [sum(rows[:k]) for k in range(pieces + 1)]
    load, n = {}, 0
    for b, block in enumerate(parts):
        for q, some in enumerate(block):
            at, load[b, q] = q * quarter, []
            for length in some:
                place = wv.at[pl.ds(at, length), pl.ds(b * HALF, HALF)]
                load[b, q].append(pltpu.make_async_copy(weights[n], place, wsem.at[n]))
                at, n = at + length, n + 1
    steps = []
    for span, loading, columns, merging in stages:
        for q in range(4):
            copies = [copy for b in loading for copy in load[b, q]]
            off = pl.multiple_of(scalars[q] * quarter, LANES)
            for k in range(*span):
                place = hv.at[pl.ds(starts[k], rows[k]), pl.ds(q * quarter, quarter)]
                source = hidden[k].at[:, pl.ds(off, quarter)]
                copies.append(pltpu.make_async_copy(source, place, hsem.at[q, k]))
                if q == 3:
                    place = tv.at[pl.ds(starts[k], rows[k]), :]
                    source = hidden[k].at[:, pl.ds(4 * quarter, LANES)]
                    copies.append(pltpu.make_async_copy(source, place, tsem.at[k]))
            steps.append((copies, q, starts[span[0]], starts[span[1]], columns, merging))
    for copies, *_ in steps[:ahead]:
        for copy in copies:
            copy.start()
    for n, (copies, q, first, stop, columns, merging) in enumerate(steps):
        for copy in copies:
            copy.wait()
        for copy in steps[n + ahead][0] if n + ahead < len(steps) else []:
            copy.start()
        here, tall = slice(first, stop), slice(0, stop - first)
        wide = slice(columns[0] * HALF, columns[1] * HALF)
        deep = slice(q * quarter, (q + 1) * quarter)
        part = jnp.dot(hv[here, deep], wv[deep, wide], preferred_element_type=jnp.float32)
        width = part.shape[1]
        if q:
            part = acc[tall, 0:width] + part
        if q < 3:
            acc[tall, 0:width] = part
            continue
        lane = lax.broadcasted_iota(jnp.int32, (stop - first, LANES), 1)
        column = lax.broadcasted_iota(jnp.int32, part.shape, 1)
        if columns[1] - columns[0] == 2:
            column = column + jnp.where(column < HALF, scalars[4], scalars[5] - HALF)
        else:
            column = column + scalars[4 + columns[0]]
        ids = tv[here, :].astype(jnp.float32)
        wanted = (ids[:, 0:1] * 256.0 + ids[:, 1:2]).astype(jnp.int32)
        top = jnp.max(part, axis=1, keepdims=True)
        if merging:
            old = prevs[0][...]
            top = jnp.maximum(top, old[:, 0:1])
        mass = jnp.sum(jnp.exp(part - top), axis=1, keepdims=True)
        found = jnp.sum(jnp.where(column == wanted, part, 0.0), axis=1, keepdims=True)
        if merging:
            mass = mass + old[:, 1:2] * jnp.exp(old[:, 0:1] - top)
            found = found + old[:, 2:3]
        row = jnp.where(lane == 0, top, jnp.where(lane == 1, mass, found))
        (out if raw else stats)[here, :] = row
    if raw:
        return
    placed, done = out.shape[0] * unit > total, 0
    if placed:
        for k in range(prev_units[0]):
            out[scalars[6 + k]] = prevs[0][k]
        done = prev_units[0]
    for k in range(total // unit):
        turned = jnp.transpose(stats[k * unit : k * unit + LANES, :])
        out[scalars[6 + done + k] if placed else k] = turned[0:8, :]


def stat_call(scalars, hidden, weights, stages, prevs, out_shape, unit, ahead):
    rows = tuple(p.shape[0] for p in hidden)
    total = sum(rows)
    tallest = max(sum(rows[span[0] : span[1]]) for span, *_ in stages)
    parts = tuple(tuple(tuple(w.shape[0] for w in some) for some in block) for block in weights)
    depth, wide = sum(n for some in parts[0] for n in some), HALF * len(parts)
    prev_units = tuple(p.shape[0] for p in prevs)
    raw = len(out_shape) == 2
    any_space = pl.BlockSpec(memory_space=pl.ANY)
    vmem = pl.BlockSpec(memory_space=pltpu.VMEM)
    loaded = [w for block in weights for some in block for w in some]
    operands = [*hidden, *loaded]
    specs = [pl.BlockSpec(memory_space=pltpu.SMEM)] + [any_space] * len(operands)
    return pl.pallas_call(
        functools.partial(stat_kernel, rows, parts, stages, prev_units, unit, ahead, raw),
        out_shape=jax.ShapeDtypeStruct(out_shape, jnp.float32),
        in_specs=specs + [vmem] * len(prevs),
        out_specs=vmem,
        scratch_shapes=[
            pltpu.VMEM((total, depth), jnp.bfloat16),
            pltpu.VMEM((total, LANES), jnp.bfloat16),
            pltpu.VMEM((depth, wide), jnp.bfloat16),
            pltpu.VMEM((tallest, wide), jnp.float32),
            pltpu.VMEM((total + LANES, LANES), jnp.float32),
            pltpu.SemaphoreType.DMA((4, len(rows))),
            pltpu.SemaphoreType.DMA((len(rows),)),
            pltpu.SemaphoreType.DMA((len(loaded),)),
        ],
        cost_estimate=pl.CostEstimate(
            flops=2 * total * depth * wide,
            bytes_accessed=2 * depth * (total + wide),
            transcendentals=total * wide,
        ),
        compiler_params=pltpu.CompilerParams(vmem_limit_bytes=56 * MIB),
    )(scalars, *operands, *prevs)


def local(hidden, head, targets):
    unit, _ = hidden.shape
    side, block, core = lax.axis_index("yh"), lax.axis_index("yl"), lax.axis_index("c")
    iz, ix = lax.axis_index("z"), lax.axis_index("x")
    ids = jnp.stack([targets // 256, targets % 256], axis=1).astype(jnp.bfloat16)
    u = jnp.concatenate([hidden, jnp.pad(ids, ((0, 0), (0, LANES - 2)))], axis=1)
    quarter = head.shape[0]
    half = quarter // 2
    mine = lax.dynamic_slice(head, (0, HALF * side), (quarter, HALF))
    low, high = (
        lax.dynamic_slice(head, (at, HALF * (1 - side)), (half, HALF)) for at in (0, half)
    )
    cut = unit // 2

    par = cross(u)
    xm, xp = shift(u, "x", 1), shift(u, "x", -1)
    zm_u, zp_u = shift(u, "z", 1), shift(u, "z", -1)
    w_near = swap(mine, "yl")
    w_far = [cross(low), cross(high)]
    w_mine_c = swap(mine, "c")

    pzm, pzp = shift(par, "z", 1), shift(par, "z", -1)
    x2 = [shift(xm[:cut], "x", 1), shift(xp[cut:], "x", -1)]
    xm_par, xp_par = shift(par, "x", 1), shift(par, "x", -1)
    zm_xm, zp_xm = shift(xm, "z", 1), shift(xm, "z", -1)

    pz2 = [shift(pzm[:cut], "z", 1), shift(pzp[cut:], "z", -1)]
    pp = jnp.concatenate([pzm, pzp])
    xm_pp, xp_pp = shift(pp, "x", 1), shift(pp, "x", -1)
    zm_xp, zp_xp = shift(xp, "z", 1), shift(xp, "z", -1)
    x2, pz2 = jnp.concatenate(x2), jnp.concatenate(pz2)
    zm_x2, zp_x2 = shift(x2, "z", 1), shift(x2, "z", -1)
    x2_par, z2_u = cross(x2), cross(pz2)
    xm_pz2, xp_pz2 = shift(pz2, "x", 1), shift(pz2, "x", -1)

    w_near_c = swap(w_near, "c")
    w_far_own = [swap(w_far[0], "yl"), swap(w_far[1], "yl")]
    w_far_c = [swap(w_far[0], "c"), swap(w_far[1], "c")]
    z2_xm = shift(zm_xm, "z", 1)
    z2_xp = cross(xp_pz2)
    x2_pp = [shift(xm_pp[:80], "x", 1), shift(xp_pp[80:], "x", -1)]
    z2_x2, x2_pz2 = shift(zp_x2, "z", -1), shift(xp_pz2, "x", -1)
    w_own_c = [swap(w_far_own[0], "c"), swap(w_far_own[1], "c")]
    own_block = [[mine], [w_mine_c], w_far_own, w_own_c]
    other_block = [[w_near], [w_near_c], w_far, w_far_c]

    early = [
        (u, [(0, 0, 0)]), (xm, [(0, -1, 0)]), (xp, [(0, 1, 0)]), (x2, [(0, 2, 0)]),
        (zm_u, [(-1, 0, 0)]), (zp_u, [(1, 0, 0)]),
        (par, [(0, 0, 1)]), (pp, [(-1, 0, 1), (1, 0, 1)]), (pz2, [(2, 0, 1)]),
        (xm_par, [(0, -1, 1)]), (xp_par, [(0, 1, 1)]),
    ]
    middle = [
        (zm_xm, [(-1, -1, 0)]), (zm_xp, [(-1, 1, 0)]), (zm_x2, [(-1, 2, 0)]),
        (zp_xm, [(1, -1, 0)]), (zp_xp, [(1, 1, 0)]), (zp_x2, [(1, 2, 0)]),
        (xm_pp, [(-1, -1, 1), (1, -1, 1)]), (xm_pz2, [(2, -1, 1)]),
        (xp_pp, [(-1, 1, 1), (1, 1, 1)]), (xp_pz2, [(2, 1, 1)]),
    ]
    early += [(x2_par, [(0, 2, 1)]), middle.pop(0), middle.pop(2)]
    middle += [(z2_u, [(2, 0, 0)])]
    late = [
        (z2_x2, [(2, 2, 0)]), (x2_pz2, [(2, 2, 1)]), (z2_xm, [(2, -1, 0)]),
        (z2_xp, [(2, 1, 0)]),
        (x2_pp[0], [(-1, 2, 1), (1, 2, 1)]), (x2_pp[1], []),
    ]
    places = jnp.array([p for _, at in early + middle + late for p in at], jnp.int32)
    slots = (iz + places[:, 0]) % 4 * 4 + (ix + places[:, 1]) % 4
    slots = slots * 2 + (block + places[:, 2]) % 2
    rank = jnp.array([[0, 0], [0, 1], [1, 0], [1, 1]], jnp.int32)
    quarters = (side + rank[:, 0]) % 2 * 2 + (core + rank[:, 1]) % 2
    base = (iz * 4 + ix) * 2 * 2 * HALF + HALF * side
    own_at, other_at = base + 2 * HALF * block, base + 2 * HALF * (1 - block)

    at = jnp.concatenate([quarters, jnp.stack([other_at, own_at]), slots]).astype(jnp.int32)
    first, second, third = ([piece for piece, _ in group] for group in (early, middle, late))
    weights, one, two = [other_block, own_block], len(first), len(second)
    rows = sum(piece.shape[0] for piece in first)
    units = (rows + sum(piece.shape[0] for piece in second)) // unit
    stages = (((0, one), (0,), (0, 1), False),)
    near = stat_call(at, first, [other_block], stages, [], (rows, LANES), unit, 2)
    stages = (((0, one), (1,), (1, 2), True), ((one, one + two), (0,), (0, 2), False))
    shape = (units, 8, LANES)
    far = stat_call(at, first + second, weights, stages, [near], shape, unit, 2)
    stages = (((0, len(third)), (0, 1), (0, 2), False),)
    stats = stat_call(at, third, weights, stages, [far], (32, 8, LANES), unit, 3)
    stats = lax.all_to_all(
        stats, ("z", "x", "yl", "yh"), 0, 0, tiled=True, axis_index_groups=PEERS
    )
    tops, masses, found = (stats[:, k, :unit] for k in range(3))
    top = jnp.max(tops, axis=0)
    mass = jnp.sum(masses * jnp.exp(tops - top), axis=0)
    return jnp.sum(found, axis=0) - (top + jnp.log(mass))


def solution(mesh):
    finer = Mesh(mesh.devices.reshape(4, 4, 2, 2, 2), AXES)
    placed = (P(AXES, None), P(("yh", "c"), ("z", "x", "yl")), P(AXES))
    return jax.shard_map(local, mesh=finer, in_specs=placed, out_specs=P(AXES), check_vma=False)
```

```python
import functools

import jax
import jax.numpy as jnp
from jax import lax
from jax.experimental import pallas as pl
from jax.experimental.pallas import tpu as pltpu
from jax.sharding import Mesh
from jax.sharding import PartitionSpec as P


AXES = ("z", "x", "yl", "yh", "c")
LANES = 128
HALF = 512
MIB = 2**20


PEERS = [[2 * k + (k + odd) % 2 for k in range(32)] for odd in (0, 1)]


def shift(x, axis, step):
    count = lax.axis_size(axis)
    return lax.ppermute(x, axis, [(k, (k + step) % count) for k in range(count)])


def swap(x, axis):
    return lax.ppermute(x, axis, [(0, 1), (1, 0)])


def cross(x):
    return lax.ppermute(x, ("yl", "yh"), [(0, 3), (3, 0), (1, 2), (2, 1)])


def stat_kernel(rows, parts, stages, prev_units, unit, ahead, raw, *refs):
    pieces, count = len(rows), len([n for block in parts for some in block for n in some])
    scalars = refs[0]
    hidden = refs[1 : 1 + pieces]
    weights = list(refs[1 + pieces : 1 + pieces + count])
    prevs = refs[1 + pieces + count : 1 + pieces + count + len(prev_units)]
    out, hv, tv, wv, acc, stats, hsem, tsem, wsem = refs[1 + pieces + count + len(prev_units) :]
    total, quarter = sum(rows), wv.shape[0] // 4
    starts = [sum(rows[:k]) for k in range(pieces + 1)]
    load, n = {}, 0
    for b, block in enumerate(parts):
        for q, some in enumerate(block):
            at, load[b, q] = q * quarter, []
            for length in some:
                place = wv.at[pl.ds(at, length), pl.ds(b * HALF, HALF)]
                load[b, q].append(pltpu.make_async_copy(weights[n], place, wsem.at[n]))
                at, n = at + length, n + 1
    steps = []
    for span, loading, columns, merging in stages:
        for q in range(4):
            copies = [copy for b in loading for copy in load[b, q]]
            off = pl.multiple_of(scalars[q] * quarter, LANES)
            for k in range(*span):
                place = hv.at[pl.ds(starts[k], rows[k]), pl.ds(q * quarter, quarter)]
                source = hidden[k].at[:, pl.ds(off, quarter)]
                copies.append(pltpu.make_async_copy(source, place, hsem.at[q, k]))
                if q == 3:
                    place = tv.at[pl.ds(starts[k], rows[k]), :]
                    source = hidden[k].at[:, pl.ds(4 * quarter, LANES)]
                    copies.append(pltpu.make_async_copy(source, place, tsem.at[k]))
            steps.append((copies, q, starts[span[0]], starts[span[1]], columns, merging))
    for copies, *_ in steps[:ahead]:
        for copy in copies:
            copy.start()
    for n, (copies, q, first, stop, columns, merging) in enumerate(steps):
        for copy in copies:
            copy.wait()
        for copy in steps[n + ahead][0] if n + ahead < len(steps) else []:
            copy.start()
        here, tall = slice(first, stop), slice(0, stop - first)
        wide = slice(columns[0] * HALF, columns[1] * HALF)
        deep = slice(q * quarter, (q + 1) * quarter)
        part = jnp.dot(hv[here, deep], wv[deep, wide], preferred_element_type=jnp.float32)
        width = part.shape[1]
        if q:
            part = acc[tall, 0:width] + part
        if q < 3:
            acc[tall, 0:width] = part
            continue
        lane = lax.broadcasted_iota(jnp.int32, (stop - first, LANES), 1)
        column = lax.broadcasted_iota(jnp.int32, part.shape, 1)
        if columns[1] - columns[0] == 2:
            column = column + jnp.where(column < HALF, scalars[4], scalars[5] - HALF)
        else:
            column = column + scalars[4 + columns[0]]
        ids = tv[here, :].astype(jnp.float32)
        wanted = (ids[:, 0:1] * 256.0 + ids[:, 1:2]).astype(jnp.int32)
        top = jnp.max(part, axis=1, keepdims=True)
        if merging:
            old = prevs[0][...]
            top = jnp.maximum(top, old[:, 0:1])
        mass = jnp.sum(jnp.exp(part - top), axis=1, keepdims=True)
        found = jnp.sum(jnp.where(column == wanted, part, 0.0), axis=1, keepdims=True)
        if merging:
            mass = mass + old[:, 1:2] * jnp.exp(old[:, 0:1] - top)
            found = found + old[:, 2:3]
        row = jnp.where(lane == 0, top, jnp.where(lane == 1, mass, found))
        (out if raw else stats)[here, :] = row
    if raw:
        return
    placed, done = out.shape[0] * unit > total, 0
    if placed:
        for k in range(prev_units[0]):
            out[scalars[6 + k]] = prevs[0][k]
        done = prev_units[0]
    for k in range(total // unit):
        turned = jnp.transpose(stats[k * unit : k * unit + LANES, :])
        out[scalars[6 + done + k] if placed else k] = turned[0:8, :]


def stat_call(scalars, hidden, weights, stages, prevs, out_shape, unit, ahead):
    rows = tuple(p.shape[0] for p in hidden)
    total = sum(rows)
    tallest = max(sum(rows[span[0] : span[1]]) for span, *_ in stages)
    parts = tuple(tuple(tuple(w.shape[0] for w in some) for some in block) for block in weights)
    depth, wide = sum(n for some in parts[0] for n in some), HALF * len(parts)
    prev_units = tuple(p.shape[0] for p in prevs)
    raw = len(out_shape) == 2
    any_space = pl.BlockSpec(memory_space=pl.ANY)
    vmem = pl.BlockSpec(memory_space=pltpu.VMEM)
    loaded = [w for block in weights for some in block for w in some]
    operands = [*hidden, *loaded]
    specs = [pl.BlockSpec(memory_space=pltpu.SMEM)] + [any_space] * len(operands)
    return pl.pallas_call(
        functools.partial(stat_kernel, rows, parts, stages, prev_units, unit, ahead, raw),
        out_shape=jax.ShapeDtypeStruct(out_shape, jnp.float32),
        in_specs=specs + [vmem] * len(prevs),
        out_specs=vmem,
        scratch_shapes=[
            pltpu.VMEM((total, depth), jnp.bfloat16),
            pltpu.VMEM((total, LANES), jnp.bfloat16),
            pltpu.VMEM((depth, wide), jnp.bfloat16),
            pltpu.VMEM((tallest, wide), jnp.float32),
            pltpu.VMEM((total + LANES, LANES), jnp.float32),
            pltpu.SemaphoreType.DMA((4, len(rows))),
            pltpu.SemaphoreType.DMA((len(rows),)),
            pltpu.SemaphoreType.DMA((len(loaded),)),
        ],
        cost_estimate=pl.CostEstimate(
            flops=2 * total * depth * wide,
            bytes_accessed=2 * depth * (total + wide),
            transcendentals=total * wide,
        ),
        compiler_params=pltpu.CompilerParams(vmem_limit_bytes=63 * MIB),
    )(scalars, *operands, *prevs)


def local(hidden, head, targets):
    unit, _ = hidden.shape
    side, block, core = lax.axis_index("yh"), lax.axis_index("yl"), lax.axis_index("c")
    iz, ix = lax.axis_index("z"), lax.axis_index("x")
    ids = jnp.stack([targets // 256, targets % 256], axis=1).astype(jnp.bfloat16)
    u = jnp.concatenate([hidden, jnp.pad(ids, ((0, 0), (0, LANES - 2)))], axis=1)
    quarter = head.shape[0]
    half = quarter // 2
    mine = lax.dynamic_slice(head, (0, HALF * side), (quarter, HALF))
    low, high = (
        lax.dynamic_slice(head, (at, HALF * (1 - side)), (half, HALF)) for at in (0, half)
    )
    cut = unit // 2

    par = cross(u)
    xm, xp = shift(u, "x", 1), shift(u, "x", -1)
    zm_u, zp_u = shift(u, "z", 1), shift(u, "z", -1)
    w_near = swap(mine, "yl")
    w_far = [cross(low), cross(high)]
    w_mine_c = swap(mine, "c")

    pzm, pzp = shift(par, "z", 1), shift(par, "z", -1)
    x2 = [shift(xm[:cut], "x", 1), shift(xp[cut:], "x", -1)]
    xm_par, xp_par = shift(par, "x", 1), shift(par, "x", -1)
    zm_xm, zp_xm = shift(xm, "z", 1), shift(xm, "z", -1)

    pz2 = [shift(pzm[:cut], "z", 1), shift(pzp[cut:], "z", -1)]
    pp = jnp.concatenate([pzm, pzp])
    xm_pp, xp_pp = shift(pp, "x", 1), shift(pp, "x", -1)
    zm_xp, zp_xp = shift(xp, "z", 1), shift(xp, "z", -1)
    x2, pz2 = jnp.concatenate(x2), jnp.concatenate(pz2)
    zm_x2, zp_x2 = shift(x2, "z", 1), shift(x2, "z", -1)
    x2_par, z2_u = cross(x2), cross(pz2)
    xm_pz2, xp_pz2 = shift(pz2, "x", 1), shift(pz2, "x", -1)

    w_near_c = swap(w_near, "c")
    w_far_own = [swap(w_far[0], "yl"), swap(w_far[1], "yl")]
    w_far_c = [swap(w_far[0], "c"), swap(w_far[1], "c")]
    z2_xm = shift(zm_xm, "z", 1)
    z2_xp = cross(xp_pz2)
    pp_a, pp_b = xm_pp[:80], xp_pp[80:]
    x2_pp = [shift(pp_a, "x", 1), shift(pp_b, "x", -1)]
    z2_x2, x2_pz2 = shift(zp_x2, "z", -1), shift(xp_pz2, "x", -1)
    w_own_c = [swap(w_far_own[0], "c"), swap(w_far_own[1], "c")]
    own_block = [[mine], [w_mine_c], w_far_own, w_own_c]
    other_block = [[w_near], [w_near_c], w_far, w_far_c]

    early = [
        (u, [(0, 0, 0)]), (xm, [(0, -1, 0)]), (xp, [(0, 1, 0)]), (x2, [(0, 2, 0)]),
        (zm_u, [(-1, 0, 0)]), (zp_u, [(1, 0, 0)]),
        (par, [(0, 0, 1)]), (pp, [(-1, 0, 1), (1, 0, 1)]), (pz2, [(2, 0, 1)]),
        (xm_par, [(0, -1, 1)]), (xp_par, [(0, 1, 1)]),
    ]
    middle = [
        (zm_xm, [(-1, -1, 0)]), (zm_xp, [(-1, 1, 0)]), (zm_x2, [(-1, 2, 0)]),
        (zp_xm, [(1, -1, 0)]), (zp_xp, [(1, 1, 0)]), (zp_x2, [(1, 2, 0)]),
        (xm_pp, [(-1, -1, 1), (1, -1, 1)]), (xm_pz2, [(2, -1, 1)]),
        (xp_pp, [(-1, 1, 1), (1, 1, 1)]), (xp_pz2, [(2, 1, 1)]),
    ]
    early += [(x2_par, [(0, 2, 1)]), middle.pop(0), middle.pop(2)]
    middle += [(z2_u, [(2, 0, 0)])]
    late = [
        (z2_x2, [(2, 2, 0)]), (x2_pz2, [(2, 2, 1)]), (z2_xm, [(2, -1, 0)]),
        (z2_xp, [(2, 1, 0)]),
        (x2_pp[0], [(-1, 2, 1), (1, 2, 1)]), (x2_pp[1], []),
    ]
    places = jnp.array([p for _, at in early + middle + late for p in at], jnp.int32)
    slots = (iz + places[:, 0]) % 4 * 4 + (ix + places[:, 1]) % 4
    slots = slots * 2 + (block + places[:, 2]) % 2
    rank = jnp.array([[0, 0], [0, 1], [1, 0], [1, 1]], jnp.int32)
    quarters = (side + rank[:, 0]) % 2 * 2 + (core + rank[:, 1]) % 2
    base = (iz * 4 + ix) * 2 * 2 * HALF + HALF * side
    own_at, other_at = base + 2 * HALF * block, base + 2 * HALF * (1 - block)

    at = jnp.concatenate([quarters, jnp.stack([other_at, own_at]), slots]).astype(jnp.int32)
    first, second, third = ([piece for piece, _ in group] for group in (early, middle, late))
    weights, one, two = [other_block, own_block], len(first), len(second)
    rows = sum(piece.shape[0] for piece in first)
    units = (rows + sum(piece.shape[0] for piece in second)) // unit
    stages = (((0, one), (0,), (0, 1), False),)
    near = stat_call(at, first, [other_block], stages, [], (rows, LANES), unit, 2)
    stages = (((0, one), (1,), (1, 2), True), ((one, one + two), (0,), (0, 2), False))
    shape = (units, 8, LANES)
    far = stat_call(at, first + second, weights, stages, [near], shape, unit, 2)
    stages = (((0, len(third)), (0, 1), (0, 2), False),)
    stats = stat_call(at, third, weights, stages, [far], (32, 8, LANES), unit, 3)
    stats = lax.all_to_all(
        stats, ("z", "x", "yl", "yh"), 0, 0, tiled=True, axis_index_groups=PEERS
    )
    tops, masses, found = (stats[:, k, :unit] for k in range(3))
    top = jnp.max(tops, axis=0)
    mass = jnp.sum(masses * jnp.exp(tops - top), axis=0)
    return jnp.sum(found, axis=0) - (top + jnp.log(mass))


def solution(mesh):
    finer = Mesh(mesh.devices.reshape(4, 4, 2, 2, 2), AXES)
    placed = (P(AXES, None), P(("yh", "c"), ("z", "x", "yl")), P(AXES))
    return jax.shard_map(local, mesh=finer, in_specs=placed, out_specs=P(AXES), check_vma=False)
```

```python
import functools

import jax
import jax.numpy as jnp
from jax import lax
from jax.experimental import pallas as pl
from jax.experimental.pallas import tpu as pltpu
from jax.sharding import Mesh
from jax.sharding import PartitionSpec as P


AXES = ("z", "x", "yl", "yh", "c")
LANES = 128
HALF = 512
MIB = 2**20


PEERS = [[2 * k + (k + odd) % 2 for k in range(32)] for odd in (0, 1)]


def shift(x, axis, step):
    count = lax.axis_size(axis)
    return lax.ppermute(x, axis, [(k, (k + step) % count) for k in range(count)])


def swap(x, axis):
    return lax.ppermute(x, axis, [(0, 1), (1, 0)])


def cross(x):
    return lax.ppermute(x, ("yl", "yh"), [(0, 3), (3, 0), (1, 2), (2, 1)])


def stat_kernel(rows, parts, stages, prev_units, unit, ahead, raw, *refs):
    pieces, count = len(rows), len([n for block in parts for some in block for n in some])
    scalars = refs[0]
    hidden = refs[1 : 1 + pieces]
    weights = list(refs[1 + pieces : 1 + pieces + count])
    prevs = refs[1 + pieces + count : 1 + pieces + count + len(prev_units)]
    out, hv, tv, wv, acc, stats, hsem, tsem, wsem = refs[1 + pieces + count + len(prev_units) :]
    total, quarter = sum(rows), wv.shape[0] // 4
    starts = [sum(rows[:k]) for k in range(pieces + 1)]
    load, n = {}, 0
    for b, block in enumerate(parts):
        for q, some in enumerate(block):
            at, load[b, q] = q * quarter, []
            for length in some:
                place = wv.at[pl.ds(at, length), pl.ds(b * HALF, HALF)]
                load[b, q].append(pltpu.make_async_copy(weights[n], place, wsem.at[n]))
                at, n = at + length, n + 1
    steps = []
    for span, loading, columns, merging in stages:
        for q in range(4):
            copies = [copy for b in loading for copy in load[b, q]]
            off = pl.multiple_of(scalars[q] * quarter, LANES)
            for k in range(*span):
                place = hv.at[pl.ds(starts[k], rows[k]), pl.ds(q * quarter, quarter)]
                source = hidden[k].at[:, pl.ds(off, quarter)]
                copies.append(pltpu.make_async_copy(source, place, hsem.at[q, k]))
                if q == 3:
                    place = tv.at[pl.ds(starts[k], rows[k]), :]
                    source = hidden[k].at[:, pl.ds(4 * quarter, LANES)]
                    copies.append(pltpu.make_async_copy(source, place, tsem.at[k]))
            steps.append((copies, q, starts[span[0]], starts[span[1]], columns, merging))
    for copies, *_ in steps[:ahead]:
        for copy in copies:
            copy.start()
    for n, (copies, q, first, stop, columns, merging) in enumerate(steps):
        for copy in copies:
            copy.wait()
        for copy in steps[n + ahead][0] if n + ahead < len(steps) else []:
            copy.start()
        here, tall = slice(first, stop), slice(0, stop - first)
        wide = slice(columns[0] * HALF, columns[1] * HALF)
        deep = slice(q * quarter, (q + 1) * quarter)
        part = jnp.dot(hv[here, deep], wv[deep, wide], preferred_element_type=jnp.float32)
        width = part.shape[1]
        if q:
            part = acc[tall, 0:width] + part
        if q < 3:
            acc[tall, 0:width] = part
            continue
        lane = lax.broadcasted_iota(jnp.int32, (stop - first, LANES), 1)
        column = lax.broadcasted_iota(jnp.int32, part.shape, 1)
        if columns[1] - columns[0] == 2:
            column = column + jnp.where(column < HALF, scalars[4], scalars[5] - HALF)
        else:
            column = column + scalars[4 + columns[0]]
        ids = tv[here, :].astype(jnp.float32)
        wanted = (ids[:, 0:1] * 256.0 + ids[:, 1:2]).astype(jnp.int32)
        top = jnp.max(part, axis=1, keepdims=True)
        if merging:
            old = prevs[0][...]
            top = jnp.maximum(top, old[:, 0:1])
        mass = jnp.sum(jnp.exp(part - top), axis=1, keepdims=True)
        found = jnp.sum(jnp.where(column == wanted, part, 0.0), axis=1, keepdims=True)
        if merging:
            mass = mass + old[:, 1:2] * jnp.exp(old[:, 0:1] - top)
            found = found + old[:, 2:3]
        row = jnp.where(lane == 0, top, jnp.where(lane == 1, mass, found))
        (out if raw else stats)[here, :] = row
    if raw:
        return
    placed, done = out.shape[0] * unit > total, 0
    if placed:
        for k in range(prev_units[0]):
            out[scalars[6 + k]] = prevs[0][k]
        done = prev_units[0]
    for k in range(total // unit):
        turned = jnp.transpose(stats[k * unit : k * unit + LANES, :])
        out[scalars[6 + done + k] if placed else k] = turned[0:8, :]


def stat_call(scalars, hidden, weights, stages, prevs, out_shape, unit, ahead):
    rows = tuple(p.shape[0] for p in hidden)
    total = sum(rows)
    tallest = max(sum(rows[span[0] : span[1]]) for span, *_ in stages)
    parts = tuple(tuple(tuple(w.shape[0] for w in some) for some in block) for block in weights)
    depth, wide = sum(n for some in parts[0] for n in some), HALF * len(parts)
    prev_units = tuple(p.shape[0] for p in prevs)
    raw = len(out_shape) == 2
    any_space = pl.BlockSpec(memory_space=pl.ANY)
    vmem = pl.BlockSpec(memory_space=pltpu.VMEM)
    loaded = [w for block in weights for some in block for w in some]
    operands = [*hidden, *loaded]
    specs = [pl.BlockSpec(memory_space=pltpu.SMEM)] + [any_space] * len(operands)
    return pl.pallas_call(
        functools.partial(stat_kernel, rows, parts, stages, prev_units, unit, ahead, raw),
        out_shape=jax.ShapeDtypeStruct(out_shape, jnp.float32),
        in_specs=specs + [vmem] * len(prevs),
        out_specs=vmem,
        scratch_shapes=[
            pltpu.VMEM((total, depth), jnp.bfloat16),
            pltpu.VMEM((total, LANES), jnp.bfloat16),
            pltpu.VMEM((depth, wide), jnp.bfloat16),
            pltpu.VMEM((tallest, wide), jnp.float32),
            pltpu.VMEM((total + LANES, LANES), jnp.float32),
            pltpu.SemaphoreType.DMA((4, len(rows))),
            pltpu.SemaphoreType.DMA((len(rows),)),
            pltpu.SemaphoreType.DMA((len(loaded),)),
        ],
        cost_estimate=pl.CostEstimate(
            flops=2 * total * depth * wide,
            bytes_accessed=2 * depth * (total + wide),
            transcendentals=total * wide,
        ),
        compiler_params=pltpu.CompilerParams(vmem_limit_bytes=63 * MIB),
    )(scalars, *operands, *prevs)


def local(hidden, head, targets):
    unit, _ = hidden.shape
    side, block, core = lax.axis_index("yh"), lax.axis_index("yl"), lax.axis_index("c")
    iz, ix = lax.axis_index("z"), lax.axis_index("x")
    ids = jnp.stack([targets // 256, targets % 256], axis=1).astype(jnp.bfloat16)
    u = jnp.concatenate([hidden, jnp.pad(ids, ((0, 0), (0, LANES - 2)))], axis=1)
    quarter = head.shape[0]
    half = quarter // 2
    mine = lax.dynamic_slice(head, (0, HALF * side), (quarter, HALF))
    low, high = (
        lax.dynamic_slice(head, (at, HALF * (1 - side)), (half, HALF)) for at in (0, half)
    )
    cut = unit // 2

    par = cross(u)
    xm, xp = shift(u, "x", 1), shift(u, "x", -1)
    zm_u, zp_u = shift(u, "z", 1), shift(u, "z", -1)
    w_near = swap(mine, "yl")
    w_far = [cross(low), cross(high)]
    w_mine_c = swap(mine, "c")

    pzm, pzp = shift(par, "z", 1), shift(par, "z", -1)
    x2 = [shift(xm[:cut], "x", 1), shift(xp[cut:], "x", -1)]
    xm_par, xp_par = shift(par, "x", 1), shift(par, "x", -1)
    zm_xm, zp_xm = shift(xm, "z", 1), shift(xm, "z", -1)

    pz2 = [shift(pzm[:cut], "z", 1), shift(pzp[cut:], "z", -1)]
    pp = jnp.concatenate([pzm, pzp])
    xm_pp, xp_pp = shift(pp, "x", 1), shift(pp, "x", -1)
    zm_xp, zp_xp = shift(xp, "z", 1), shift(xp, "z", -1)
    x2, pz2 = jnp.concatenate(x2), jnp.concatenate(pz2)
    zm_x2, zp_x2 = shift(x2, "z", 1), shift(x2, "z", -1)
    x2_par, z2_u = cross(x2), cross(pz2)
    xm_pz2, xp_pz2 = shift(pz2, "x", 1), shift(pz2, "x", -1)

    w_near_c = swap(w_near, "c")
    w_far_own = [swap(w_far[0], "yl"), swap(w_far[1], "yl")]
    w_far_c = [swap(w_far[0], "c"), swap(w_far[1], "c")]
    z2_xm = shift(zm_xm, "z", 1)
    z2_xp = cross(xp_pz2)
    x2_pp = shift(xm_pp, "x", 1)
    z2_x2, x2_pz2 = shift(zp_x2, "z", -1), shift(xp_pz2, "x", -1)
    w_own_c = [swap(w_far_own[0], "c"), swap(w_far_own[1], "c")]
    own_block = [[mine], [w_mine_c], w_far_own, w_own_c]
    other_block = [[w_near], [w_near_c], w_far, w_far_c]

    early = [
        (u, [(0, 0, 0)]), (xm, [(0, -1, 0)]), (xp, [(0, 1, 0)]), (x2, [(0, 2, 0)]),
        (zm_u, [(-1, 0, 0)]), (zp_u, [(1, 0, 0)]),
        (par, [(0, 0, 1)]), (pp, [(-1, 0, 1), (1, 0, 1)]), (pz2, [(2, 0, 1)]),
        (xm_par, [(0, -1, 1)]), (xp_par, [(0, 1, 1)]),
    ]
    middle = [
        (zm_xm, [(-1, -1, 0)]), (zm_xp, [(-1, 1, 0)]), (zm_x2, [(-1, 2, 0)]),
        (zp_xm, [(1, -1, 0)]), (zp_xp, [(1, 1, 0)]), (zp_x2, [(1, 2, 0)]),
        (xm_pp, [(-1, -1, 1), (1, -1, 1)]), (xm_pz2, [(2, -1, 1)]),
        (xp_pp, [(-1, 1, 1), (1, 1, 1)]), (xp_pz2, [(2, 1, 1)]),
    ]
    early += [middle.pop(0), middle.pop(2)]
    middle += [(x2_par, [(0, 2, 1)]), (z2_u, [(2, 0, 0)])]
    late = [
        (z2_x2, [(2, 2, 0)]), (x2_pz2, [(2, 2, 1)]), (z2_xm, [(2, -1, 0)]),
        (z2_xp, [(2, 1, 0)]),
        (x2_pp, [(-1, 2, 1), (1, 2, 1)]),
    ]
    places = jnp.array([p for _, at in early + middle + late for p in at], jnp.int32)
    slots = (iz + places[:, 0]) % 4 * 4 + (ix + places[:, 1]) % 4
    slots = slots * 2 + (block + places[:, 2]) % 2
    rank = jnp.array([[0, 0], [0, 1], [1, 0], [1, 1]], jnp.int32)
    quarters = (side + rank[:, 0]) % 2 * 2 + (core + rank[:, 1]) % 2
    base = (iz * 4 + ix) * 2 * 2 * HALF + HALF * side
    own_at, other_at = base + 2 * HALF * block, base + 2 * HALF * (1 - block)

    at = jnp.concatenate([quarters, jnp.stack([other_at, own_at]), slots]).astype(jnp.int32)
    first, second, third = ([piece for piece, _ in group] for group in (early, middle, late))
    weights, one, two = [other_block, own_block], len(first), len(second)
    rows = sum(piece.shape[0] for piece in first)
    units = (rows + sum(piece.shape[0] for piece in second)) // unit
    stages = (((0, one), (0,), (0, 1), False),)
    near = stat_call(at, first, [other_block], stages, [], (rows, LANES), unit, 2)
    stages = (((one, one + two), (0, 1), (0, 2), False), ((0, one), (), (1, 2), True))
    shape = (units, 8, LANES)
    far = stat_call(at, first + second, weights, stages, [near], shape, unit, 2)
    stages = (((0, len(third)), (0, 1), (0, 2), False),)
    stats = stat_call(at, third, weights, stages, [far], (32, 8, LANES), unit, 3)
    stats = lax.all_to_all(
        stats, ("z", "x", "yl", "yh"), 0, 0, tiled=True, axis_index_groups=PEERS
    )
    tops, masses, found = (stats[:, k, :unit] for k in range(3))
    top = jnp.max(tops, axis=0)
    mass = jnp.sum(masses * jnp.exp(tops - top), axis=0)
    return jnp.sum(found, axis=0) - (top + jnp.log(mass))


def solution(mesh):
    finer = Mesh(mesh.devices.reshape(4, 4, 2, 2, 2), AXES)
    placed = (P(AXES, None), P(("yh", "c"), ("z", "x", "yl")), P(AXES))
    return jax.shard_map(local, mesh=finer, in_specs=placed, out_specs=P(AXES), check_vma=False)
```

```python
import functools

import jax
import jax.numpy as jnp
from jax import lax
from jax.experimental import pallas as pl
from jax.experimental.pallas import tpu as pltpu
from jax.sharding import Mesh
from jax.sharding import PartitionSpec as P


AXES = ("z", "x", "yl", "yh", "c")
LANES = 128
HALF = 512
MIB = 2**20


PEERS = [[2 * k + (k + odd) % 2 for k in range(32)] for odd in (0, 1)]


def shift(x, axis, step):
    count = lax.axis_size(axis)
    return lax.ppermute(x, axis, [(k, (k + step) % count) for k in range(count)])


def swap(x, axis):
    return lax.ppermute(x, axis, [(0, 1), (1, 0)])


def cross(x):
    return lax.ppermute(x, ("yl", "yh"), [(0, 3), (3, 0), (1, 2), (2, 1)])


def stat_kernel(rows, parts, stages, prevs_units, unit, ahead, outs, *refs):
    pieces, count = len(rows), len([n for block in parts for some in block for n in some])
    scalars = refs[0]
    hidden = refs[1 : 1 + pieces]
    weights = list(refs[1 + pieces : 1 + pieces + count])
    prevs = refs[1 + pieces + count : 1 + pieces + count + len(prevs_units)]
    rest = refs[1 + pieces + count + len(prevs_units) :]
    out, (hv, tv, wv, acc, stats, hsem, tsem, wsem) = rest[0], rest[outs:]
    raw = outs == 2
    total, quarter = sum(rows), wv.shape[0] // 4
    starts = [sum(rows[:k]) for k in range(pieces + 1)]
    load, n = {}, 0
    for b, block in enumerate(parts):
        for q, some in enumerate(block):
            at, load[b, q] = q * quarter, []
            for length in some:
                place = wv.at[pl.ds(at, length), pl.ds(b * HALF, HALF)]
                load[b, q].append(pltpu.make_async_copy(weights[n], place, wsem.at[n]))
                at, n = at + length, n + 1
    steps = []
    for span, bring, loading, columns, quarters, kind in stages:
        for q in quarters:
            copies = [copy for b in loading for copy in load[b, q]]
            off = pl.multiple_of(scalars[q] * quarter, LANES)
            for k in range(*span) if bring else ():
                place = hv.at[pl.ds(starts[k], rows[k]), pl.ds(q * quarter, quarter)]
                source = hidden[k].at[:, pl.ds(off, quarter)]
                copies.append(pltpu.make_async_copy(source, place, hsem.at[q, k]))
                if q == 3:
                    place = tv.at[pl.ds(starts[k], rows[k]), :]
                    source = hidden[k].at[:, pl.ds(4 * quarter, LANES)]
                    copies.append(pltpu.make_async_copy(source, place, tsem.at[k]))
            ends = (q == quarters[0], q == quarters[-1])
            steps.append((copies, q, starts[span[0]], starts[span[1]], columns, kind, ends))
    for copies, *_ in steps[:ahead]:
        for copy in copies:
            copy.start()
    for n, (copies, q, first, stop, columns, kind, ends) in enumerate(steps):
        for copy in copies:
            copy.wait()
        for copy in steps[n + ahead][0] if n + ahead < len(steps) else []:
            copy.start()
        merging = kind == "add"
        here, tall = slice(first, stop), slice(0, stop - first)
        wide = slice(columns[0] * HALF, columns[1] * HALF)
        deep = slice(q * quarter, (q + 1) * quarter)
        part = jnp.dot(hv[here, deep], wv[deep, wide], preferred_element_type=jnp.float32)
        width = part.shape[1]
        if not ends[0]:
            part = acc[tall, 0:width] + part
        elif merging:
            part = prevs[1][...] + part
        if not ends[1]:
            acc[tall, 0:width] = part
            continue
        if kind == "keep":
            rest[1][...] = part
            continue
        lane = lax.broadcasted_iota(jnp.int32, (stop - first, LANES), 1)
        column = lax.broadcasted_iota(jnp.int32, part.shape, 1)
        if columns[1] - columns[0] == 2:
            column = column + jnp.where(column < HALF, scalars[4], scalars[5] - HALF)
        else:
            column = column + scalars[4 + columns[0]]
        ids = tv[here, :].astype(jnp.float32)
        wanted = (ids[:, 0:1] * 256.0 + ids[:, 1:2]).astype(jnp.int32)
        top = jnp.max(part, axis=1, keepdims=True)
        if merging:
            old = prevs[0][...]
            top = jnp.maximum(top, old[:, 0:1])
        mass = jnp.sum(jnp.exp(part - top), axis=1, keepdims=True)
        found = jnp.sum(jnp.where(column == wanted, part, 0.0), axis=1, keepdims=True)
        if merging:
            mass = mass + old[:, 1:2] * jnp.exp(old[:, 0:1] - top)
            found = found + old[:, 2:3]
        row = jnp.where(lane == 0, top, jnp.where(lane == 1, mass, found))
        (out if raw else stats)[here, :] = row
    if raw:
        return
    placed, done = out.shape[0] * unit > total, 0
    if placed:
        for k in range(prevs_units[0]):
            out[scalars[6 + k]] = prevs[0][k]
        done = prevs_units[0]
    for k in range(total // unit):
        turned = jnp.transpose(stats[k * unit : k * unit + LANES, :])
        out[scalars[6 + done + k] if placed else k] = turned[0:8, :]


def stat_call(scalars, hidden, weights, stages, prevs, out_shapes, unit, ahead):
    rows = tuple(p.shape[0] for p in hidden)
    total = sum(rows)
    tallest = max(sum(rows[span[0] : span[1]]) for span, *_ in stages)
    parts = tuple(tuple(tuple(w.shape[0] for w in some) for some in block) for block in weights)
    depth, wide = sum(n for some in parts[0] for n in some), HALF * len(parts)
    prev_units = tuple(p.shape[0] for p in prevs)
    outs = len(out_shapes)
    any_space = pl.BlockSpec(memory_space=pl.ANY)
    vmem = pl.BlockSpec(memory_space=pltpu.VMEM)
    loaded = [w for block in weights for some in block for w in some]
    operands = [*hidden, *loaded]
    specs = [pl.BlockSpec(memory_space=pltpu.SMEM)] + [any_space] * len(operands)
    return pl.pallas_call(
        functools.partial(stat_kernel, rows, parts, stages, prev_units, unit, ahead, outs),
        out_shape=[jax.ShapeDtypeStruct(shape, jnp.float32) for shape in out_shapes],
        in_specs=specs + [vmem] * len(prevs),
        out_specs=[vmem] * outs,
        scratch_shapes=[
            pltpu.VMEM((total, depth), jnp.bfloat16),
            pltpu.VMEM((total, LANES), jnp.bfloat16),
            pltpu.VMEM((depth, wide), jnp.bfloat16),
            pltpu.VMEM((tallest, wide), jnp.float32),
            pltpu.VMEM((total + LANES, LANES), jnp.float32),
            pltpu.SemaphoreType.DMA((4, len(rows))),
            pltpu.SemaphoreType.DMA((len(rows),)),
            pltpu.SemaphoreType.DMA((len(loaded),)),
        ],
        cost_estimate=pl.CostEstimate(
            flops=2 * total * depth * wide,
            bytes_accessed=2 * depth * (total + wide),
            transcendentals=total * wide,
        ),
        compiler_params=pltpu.CompilerParams(vmem_limit_bytes=63 * MIB),
    )(scalars, *operands, *prevs)


def local(hidden, head, targets):
    unit, _ = hidden.shape
    side, block, core = lax.axis_index("yh"), lax.axis_index("yl"), lax.axis_index("c")
    iz, ix = lax.axis_index("z"), lax.axis_index("x")
    ids = jnp.stack([targets // 256, targets % 256], axis=1).astype(jnp.bfloat16)
    u = jnp.concatenate([hidden, jnp.pad(ids, ((0, 0), (0, LANES - 2)))], axis=1)
    quarter = head.shape[0]
    half = quarter // 2
    mine = lax.dynamic_slice(head, (0, HALF * side), (quarter, HALF))
    low, high = (
        lax.dynamic_slice(head, (at, HALF * (1 - side)), (half, HALF)) for at in (0, half)
    )
    cut = unit // 2

    par = cross(u)
    xm, xp = shift(u, "x", 1), shift(u, "x", -1)
    zm_u, zp_u = shift(u, "z", 1), shift(u, "z", -1)
    w_near = swap(mine, "yl")
    w_far = [cross(low), cross(high)]
    w_mine_c = swap(mine, "c")

    pzm, pzp = shift(par, "z", 1), shift(par, "z", -1)
    x2 = [shift(xm[:cut], "x", 1), shift(xp[cut:], "x", -1)]
    xm_par, xp_par = shift(par, "x", 1), shift(par, "x", -1)
    zm_xm, zp_xm = shift(xm, "z", 1), shift(xm, "z", -1)

    pz2 = [shift(pzm[:cut], "z", 1), shift(pzp[cut:], "z", -1)]
    pp = jnp.concatenate([pzm, pzp])
    xm_pp, xp_pp = shift(pp, "x", 1), shift(pp, "x", -1)
    zm_xp, zp_xp = shift(xp, "z", 1), shift(xp, "z", -1)
    x2, pz2 = jnp.concatenate(x2), jnp.concatenate(pz2)
    zm_x2, zp_x2 = shift(x2, "z", 1), shift(x2, "z", -1)
    x2_par, z2_u = cross(x2), cross(pz2)
    xm_pz2, xp_pz2 = shift(pz2, "x", 1), shift(pz2, "x", -1)

    w_near_c = swap(w_near, "c")
    w_far_own = [swap(w_far[0], "yl"), swap(w_far[1], "yl")]
    w_far_c = [swap(w_far[0], "c"), swap(w_far[1], "c")]
    z2_xm = shift(zm_xm, "z", 1)
    z2_xp = cross(xp_pz2)
    zm_x2p, zp_x2p = shift(x2_par, "z", 1), shift(x2_par, "z", -1)
    z2_x2, x2_pz2 = shift(zp_x2, "z", -1), shift(xp_pz2, "x", -1)
    w_own_c = [swap(w_far_own[0], "c"), swap(w_far_own[1], "c")]
    own_block = [[mine], [w_mine_c], w_far_own, w_own_c]
    other_block = [[w_near], [w_near_c], w_far, w_far_c]

    early = [
        (u, [(0, 0, 0)]), (xm, [(0, -1, 0)]), (xp, [(0, 1, 0)]), (x2, [(0, 2, 0)]),
        (zm_u, [(-1, 0, 0)]), (zp_u, [(1, 0, 0)]),
        (par, [(0, 0, 1)]), (pp, [(-1, 0, 1), (1, 0, 1)]), (pz2, [(2, 0, 1)]),
        (xm_par, [(0, -1, 1)]), (xp_par, [(0, 1, 1)]),
    ]
    middle = [
        (zm_xm, [(-1, -1, 0)]), (zm_xp, [(-1, 1, 0)]), (zm_x2, [(-1, 2, 0)]),
        (zp_xm, [(1, -1, 0)]), (zp_xp, [(1, 1, 0)]), (zp_x2, [(1, 2, 0)]),
        (xm_pp, [(-1, -1, 1), (1, -1, 1)]), (xm_pz2, [(2, -1, 1)]),
        (xp_pp, [(-1, 1, 1), (1, 1, 1)]), (xp_pz2, [(2, 1, 1)]),
    ]
    early += [middle.pop(0), middle.pop(2)]
    middle += [(x2_par, [(0, 2, 1)]), (z2_u, [(2, 0, 0)])]
    late = [
        (z2_x2, [(2, 2, 0)]), (x2_pz2, [(2, 2, 1)]), (z2_xm, [(2, -1, 0)]),
        (z2_xp, [(2, 1, 0)]),
        (zm_x2p, [(-1, 2, 1)]), (zp_x2p, [(1, 2, 1)]),
    ]
    places = jnp.array([p for _, at in early + middle + late for p in at], jnp.int32)
    slots = (iz + places[:, 0]) % 4 * 4 + (ix + places[:, 1]) % 4
    slots = slots * 2 + (block + places[:, 2]) % 2
    rank = jnp.array([[0, 0], [0, 1], [1, 0], [1, 1]], jnp.int32)
    quarters = (side + rank[:, 0]) % 2 * 2 + (core + rank[:, 1]) % 2
    base = (iz * 4 + ix) * 2 * 2 * HALF + HALF * side
    own_at, other_at = base + 2 * HALF * block, base + 2 * HALF * (1 - block)

    at = jnp.concatenate([quarters, jnp.stack([other_at, own_at]), slots]).astype(jnp.int32)
    first, second, third = ([piece for piece, _ in group] for group in (early, middle, late))
    weights, one, two = [other_block, own_block], len(first), len(second)
    rows = sum(piece.shape[0] for piece in first)
    units = (rows + sum(piece.shape[0] for piece in second)) // unit
    every = (0, 1, 2, 3)
    stages = (
        ((0, one), True, (0,), (0, 1), every, "new"),
        ((0, one), False, (1,), (1, 2), (0, 1), "keep"),
    )
    shapes, some = [(rows, LANES), (rows, HALF)], [other_block, own_block[:2]]
    near = stat_call(at, first, some, stages, [], shapes, unit, 2)
    stages = (
        ((one, one + two), True, (0, 1), (0, 2), every, "new"),
        ((0, one), True, (), (1, 2), (2, 3), "add"),
    )
    shapes = [(units, 8, LANES)]
    far = stat_call(at, first + second, weights, stages, near, shapes, unit, 2)
    stages = (((0, len(third)), True, (0, 1), (0, 2), every, "new"),)
    stats = stat_call(at, third, weights, stages, far, [(32, 8, LANES)], unit, 3)[0]
    stats = lax.all_to_all(
        stats, ("z", "x", "yl", "yh"), 0, 0, tiled=True, axis_index_groups=PEERS
    )
    tops, masses, found = (stats[:, k, :unit] for k in range(3))
    top = jnp.max(tops, axis=0)
    mass = jnp.sum(masses * jnp.exp(tops - top), axis=0)
    return jnp.sum(found, axis=0) - (top + jnp.log(mass))


def solution(mesh):
    finer = Mesh(mesh.devices.reshape(4, 4, 2, 2, 2), AXES)
    placed = (P(AXES, None), P(("yh", "c"), ("z", "x", "yl")), P(AXES))
    return jax.shard_map(local, mesh=finer, in_specs=placed, out_specs=P(AXES), check_vma=False)
```
